128 devices in a mesh: ep: 32 (over y, x, core), dp: 4 (over z).
Axes of the slice: x: 4, y: 4, z: 4, core: 2. Of those that a mesh axis runs over, the one named last changes fastest.
Arguments:
- resid: bfloat16 [2048, 4096], P(('ep', 'dp')), may hold values from -6 to 6
- queries: bfloat16 [2048, 8192], P(('ep', 'dp')), may hold values from -4.5 to 4.5
- new_keys: bfloat16 [2048, 512], P(('ep', 'dp')), may hold values from -4.5 to 4.5
- new_values: bfloat16 [2048, 512], P(('ep', 'dp')), may hold values from -6 to 6
- cache_keys: bfloat16 [2048, 128, 512], P(('ep', 'dp')), may hold values from -4.5 to 4.5
- cache_values: bfloat16 [2048, 128, 512], P(('ep', 'dp')), may hold values from -6 to 6
- cache_len: int32 [2048], P(('ep', 'dp')), may hold values from 1 to 128
- out_proj: bfloat16 [8192, 4096], P('ep'), may hold values from -0.0625 to 0.0625
- norm_gain: float32 [4096], replicated, may hold values from 0.1 to 1.9
- router: bfloat16 [4096, 64], replicated, may hold values from -4 to 4
- expert_ids: int32 [2048, 8], P(('ep', 'dp')), may hold values from 0 to 63, all different within a row; in each aligned block of 16 rows (0 to 15, 16 to 31, ...) at most 4 rows name the same one
- gate_slab: bfloat16 [128, 4096, 384], P(('ep', 'dp')), may hold values from -0.09375 to 0.09375
- up_slab: bfloat16 [128, 4096, 384], P(('ep', 'dp')), may hold values from -0.09375 to 0.09375
- down_slab: bfloat16 [128, 384, 4096], P(('ep', 'dp')), may hold values from -0.21875 to 0.21875
Outputs:
- mixed: float32 [2048, 4096], P(('ep', 'dp'))
The draws below stay inside these ranges and needn't reach their ends.
Inputs may be any that keep to these rules, and one draw needn't show every extreme that they name: `expert_ids`: each row names 8 different experts; among the rows of one device no expert is named by more than 4 rows.
All inputs are finite; a program needn't handle non-finite values.
Results may differ from the reference program's by a relative error of at most 0.009.
Values may be sent and summed in bfloat16 or wider, within the bound.
A program may use at most 128 MiB of HBM per device.

```python
import math
import jax
import jax.numpy as jnp
import numpy as np
from jax import lax

D = 4096
H = 64
KVH = 4
HD = 128
TOP = 8
FF = 768
TOK_DEV = 16
CACHE = 128
EXPERTS = 64
HF = 384
CAP = 4
TOKENS = 2048
N_EP = 32
DEVICES = 128


edge_value = 4.5


def draw_queries(key, part):
    sampled = jnp.clip(jax.random.normal(jax.random.fold_in(key, 1), (TOKENS, H * HD), jnp.float32), -edge_value, edge_value)
    return sampled.astype(jnp.bfloat16)


def draw_cache_keys(key, part):
    sampled = jnp.clip(jax.random.normal(jax.random.fold_in(key, 2), (TOKENS, CACHE, KVH * HD), jnp.float32), -edge_value, edge_value)
    return sampled.astype(jnp.bfloat16)


def draw_router(key, part):
    sampled = jnp.clip(jax.random.normal(jax.random.fold_in(key, 3), (D, EXPERTS), jnp.float32), -4.0, 4.0) / math.sqrt(D)
    return sampled.astype(jnp.bfloat16)


def with_ends(entries, own_key, low, high):
    place = [jax.random.randint(jax.random.fold_in(own_key, axis), (), 0, length) for axis, length in enumerate(entries.shape)]
    main_axis = entries.shape.index(max(entries.shape))
    neighbour = place[:main_axis] + [(place[main_axis] + 1) % entries.shape[main_axis]] + place[main_axis + 1:]
    return entries.at[tuple(place)].set(low).at[tuple(neighbour)].set(high)


def shard_levels(rng, shape, split, least, high):
    loudness, own = 1.0, jax.random.fold_in(rng, 6)
    for axis_at, parts in split:
        steps = jnp.exp(jax.random.uniform(jax.random.fold_in(own, axis_at), (parts,), jnp.float32, least / len(split), high / len(split)))
        loudness = loudness * jnp.repeat(steps, shape[axis_at] // parts).reshape([-1 if axis == axis_at else 1 for axis in range(len(shape))])
    return loudness


def assign_block(rng, own, number, rows, number_of, top, reach, lean):
    order = jax.random.permutation(rng, number_of)
    heavy_load, ordinary = portions_of(number_of, rows * top, reach, lean, True), portions_of(number_of, rows * top, reach, lean, False)
    places = jnp.arange(number_of)

    def named(sizes, offset_by):
        used = int((sizes > 0).sum())
        fixed = max(1, used // 4)
        passed = fixed + (places - fixed + offset_by * (used - fixed)) % max(1, number_of - fixed)
        return jnp.zeros((number_of,), jnp.int32).at[order[jnp.where(places < fixed, places, passed)]].set(jnp.asarray(sizes, jnp.int32))

    sizes = jnp.where(number % 4 == 0, named(heavy_load, number // 4), named(ordinary, number - number // 4 - 1))
    mixed = jax.random.permutation(jax.random.fold_in(own, 3), number_of)
    donor, sink = mixed[0:number_of // 2 * 2:2], mixed[1:number_of // 2 * 2:2]
    margin = jnp.minimum(sizes[donor] - 1, reach - sizes[sink]) // 2
    margin = jnp.where((donor == order[0]) | (sink == order[0]) | (sizes[sink] == 0), 0, jnp.maximum(margin, 0))
    passed = jax.random.randint(jax.random.fold_in(own, 4), (number_of // 2,), 0, 1 << 20) % (margin + 1)
    sizes = sizes.at[donor].add(-passed).at[sink].add(passed)
    labels = jnp.searchsorted(jnp.cumsum(sizes), jnp.arange(rows * top), side="right").astype(jnp.int32)
    listing = labels.reshape(top, rows).T
    listing = listing[jax.random.permutation(jax.random.fold_in(own, 1), rows)]
    offset_by = jax.random.randint(jax.random.fold_in(own, 2), (rows, 1), 0, top)
    return jnp.take_along_axis(listing, (jnp.arange(top)[None, :] + offset_by) % top, axis=1)


def portions_of(count, total, limit, skew, full):
    portions = [(1 << 20) // math.isqrt(rank ** skew) + 1 for rank in range(1, count + 1)]
    largest = limit if full else min(limit, max(-(-total // count), total * portions[0] // sum(portions)))
    least = 1 if total - largest >= count - 1 else 0
    given, spare = [largest] + [least] * (count - 1), total - largest - least * (count - 1)
    while spare > 0:
        movable = [i for i in range(1, count) if given[i] < largest] or [i for i in range(1, count) if given[i] < limit]
        mass, left = sum([portions[i] for i in movable]), spare
        for i in movable:
            addition = min(limit - given[i], max(1, left * portions[i] // mass), spare)
            given[i] = given[i] + addition
            spare = spare - addition
    return np.array(given)


def scatter_about(key, dims, width, reach, cuts=(), held_as=jnp.bfloat16):
    values = width * jax.random.normal(key, dims, jnp.float32)
    if cuts:
        values = values * shard_levels(key, dims, cuts, -0.22, 0.18)
    return jnp.clip(values, -reach, reach).astype(held_as)


def setup_inputs(seed: int = 0) -> dict:
    seeds = jax.random.split(jax.random.key(seed), 15)
    resid = scatter_about(seeds[0], (TOKENS, D), 1.0, 6.0, ((0, 128),))
    queries = draw_queries(jax.random.fold_in(seeds[14], 71), 0)
    new_keys = scatter_about(seeds[2], (TOKENS, KVH * HD), 1.0, 4.5, ((0, 128),))
    new_values = scatter_about(seeds[3], (TOKENS, KVH * HD), 1.0, 6.0, ((0, 128),))
    cache_keys = draw_cache_keys(jax.random.fold_in(seeds[14], 71), 0)
    cache_values = scatter_about(seeds[5], (TOKENS, CACHE, KVH * HD), 1.0, 6.0, ((0, 128),))
    cache_len = with_ends(jax.random.randint(seeds[6], (TOKENS,), 1, CACHE + 1), jax.random.fold_in(seeds[6], 1), 1, CACHE).astype(jnp.int32)
    out_proj = scatter_about(seeds[7], (H * HD, D), (H * HD) ** -0.5, 0.0625, ((0, 32),))
    norm_gain = jnp.clip(1.0 + 0.18 * jax.random.normal(seeds[8], (D,), jnp.float32), 0.1, 1.9)
    router = draw_router(jax.random.fold_in(seeds[14], 71), 0)
    expert_ids_keys = jax.random.split(jax.random.fold_in(seeds[10], 1), TOKENS // TOK_DEV)
    expert_ids_turns = jax.random.permutation(jax.random.fold_in(seeds[10], 3), TOKENS // TOK_DEV)
    expert_ids = jax.vmap(lambda own, number: assign_block(jax.random.fold_in(seeds[10], 2), own, number, TOK_DEV, EXPERTS, TOP, CAP, 2))(expert_ids_keys, expert_ids_turns).reshape((TOKENS, TOP))
    gate_slab = scatter_about(seeds[11], (DEVICES, D, HF), D ** -0.5, 0.09375, ((0, 128),))
    up_slab = scatter_about(seeds[12], (DEVICES, D, HF), D ** -0.5, 0.09375, ((0, 128),))
    down_slab = scatter_about(seeds[13], (DEVICES, HF, D), FF ** -0.5, 0.21875, ((0, 128),))
    return {"resid": resid, "queries": queries, "new_keys": new_keys, "new_values": new_values, "cache_keys": cache_keys, "cache_values": cache_values, "cache_len": cache_len, "out_proj": out_proj, "norm_gain": norm_gain, "router": router, "expert_ids": expert_ids, "gate_slab": gate_slab, "up_slab": up_slab, "down_slab": down_slab}


def attend_block(query_rows, key_new, value_new, key_cache, value_cache, lengths):
    local_rows = query_rows.shape[0]
    cache_span = key_cache.shape[1]
    group_size = H // KVH
    query_heads = query_rows.astype(jnp.float32).reshape(local_rows, KVH, group_size, HD)
    past_keys = key_cache.astype(jnp.float32).reshape(local_rows, cache_span, KVH, HD)
    past_values = value_cache.astype(jnp.float32).reshape(local_rows, cache_span, KVH, HD)
    score_scale = 1.0 / math.sqrt(HD)
    past_scores = jnp.einsum('tgqd,tcgd->tgqc', query_heads, past_keys) * score_scale
    own_scores = jnp.einsum('tgqd,tgd->tgq', query_heads, key_new.astype(jnp.float32).reshape(local_rows, KVH, HD)) * score_scale
    is_valid = lax.broadcasted_iota(jnp.int32, (local_rows, cache_span), 1) < lengths[:, None]
    past_scores = jnp.where(is_valid[:, None, None, :], past_scores, -1e+30)
    peak_score = jnp.maximum(lax.optimization_barrier(jnp.max(past_scores, axis=3)), own_scores)
    past_exp = jnp.exp(past_scores - peak_score[..., None])
    own_exp = jnp.exp(own_scores - peak_score)
    denom_sum = lax.optimization_barrier(jnp.sum(past_exp, axis=3)) + own_exp
    past_weights = lax.optimization_barrier((past_exp / denom_sum[..., None]).astype(jnp.bfloat16))
    own_weights = lax.optimization_barrier((own_exp / denom_sum).astype(jnp.bfloat16))
    blended = jnp.einsum('tgqc,tcgd->tgqd', past_weights.astype(jnp.float32), past_values)
    blended = blended + own_weights.astype(jnp.float32)[..., None] * value_new.astype(jnp.float32).reshape(local_rows, KVH, 1, HD)
    return blended.reshape(local_rows, H * HD).astype(jnp.bfloat16)

def attend_packed(packed):
    return attend_block(*packed)

def blocked(array):
    return array.reshape((DEVICES, TOK_DEV) + array.shape[1:])

def reference(resid, queries, new_keys, new_values, cache_keys, cache_values, cache_len, out_proj, norm_gain, router, expert_ids, gate_slab, up_slab, down_slab):
    packed = (blocked(queries), blocked(new_keys), blocked(new_values), blocked(cache_keys), blocked(cache_values), blocked(cache_len))
    attended = lax.map(attend_packed, packed).reshape(TOKENS, H * HD)
    column_width = H * HD // N_EP
    attn_out = jnp.zeros((TOKENS, D), jnp.float32)
    for shard_index in range(N_EP):
        row_start = shard_index * column_width
        product = jnp.dot(attended[:, row_start:row_start + column_width], out_proj[row_start:row_start + column_width], preferred_element_type=jnp.float32)
        rounded = lax.optimization_barrier(product.astype(jnp.bfloat16))
        attn_out = attn_out + rounded.astype(jnp.float32)
    hidden = resid.astype(jnp.float32) + attn_out
    meansq = lax.optimization_barrier(jnp.mean(hidden * hidden, axis=1, keepdims=True))
    normed = (hidden * lax.rsqrt(jnp.maximum(meansq, 0.25)) * norm_gain).astype(jnp.bfloat16)
    logits = jnp.dot(normed, router, preferred_element_type=jnp.float32)
    chosen = jnp.take_along_axis(logits, expert_ids.astype(jnp.int32), axis=1)
    peak_logit = lax.optimization_barrier(jnp.max(chosen, axis=1, keepdims=True))
    exp_logit = jnp.exp(chosen - peak_logit)
    gate_probs = lax.optimization_barrier((exp_logit / lax.optimization_barrier(jnp.sum(exp_logit, axis=1, keepdims=True))).astype(jnp.bfloat16))
    flat_ids = expert_ids.reshape(-1).astype(jnp.int32)
    token_of = (jnp.arange(TOKENS * TOP, dtype=jnp.int32) // TOP).astype(jnp.int32)
    onehot = (flat_ids[:, None] == jnp.arange(EXPERTS, dtype=jnp.int32)[None, :]).astype(jnp.int32)
    earlier = jnp.cumsum(onehot, axis=0).astype(jnp.int32) - onehot
    ranking = lax.optimization_barrier(jnp.sum(earlier * onehot, axis=1)).astype(jnp.int32)
    row_depth = DEVICES * CAP
    row_table = jnp.zeros((EXPERTS, row_depth), jnp.int32).at[flat_ids, ranking].set(token_of)

    def run_expert(expert):
        rows_in = jnp.take(normed, row_table[expert], axis=0)
        gate_full = jnp.concatenate((gate_slab[2 * expert], gate_slab[2 * expert + 1]), axis=1)
        up_full = jnp.concatenate((up_slab[2 * expert], up_slab[2 * expert + 1]), axis=1)
        down_full = jnp.concatenate((down_slab[2 * expert], down_slab[2 * expert + 1]), axis=0)
        gate_val = jnp.dot(rows_in, gate_full, preferred_element_type=jnp.float32)
        up_val = jnp.dot(rows_in, up_full, preferred_element_type=jnp.float32)
        activated = (jax.nn.silu(gate_val) * up_val).astype(jnp.bfloat16)
        return jnp.dot(activated, down_full, preferred_element_type=jnp.float32).astype(jnp.bfloat16)
    produced = lax.map(run_expert, jnp.arange(EXPERTS, dtype=jnp.int32))
    picked = produced[flat_ids, ranking].reshape(TOKENS, TOP, D)
    expert_mix = jnp.einsum('tk,tkd->td', gate_probs.astype(jnp.float32), picked.astype(jnp.float32))
    return hidden + expert_mix
```

```python
import math

import jax
import jax.numpy as jnp
from jax import lax
from jax.experimental import pallas as pl
from jax.experimental.pallas import tpu as pltpu
from jax.sharding import PartitionSpec as P

D = 4096
H = 64
KVH = 4
HD = 128
TOP = 8


def attend(queries, new_keys, new_values, cache_keys, cache_values, cache_len):
    local_rows = queries.shape[0]
    cache_span = cache_keys.shape[1]
    group_size = H // KVH
    query_heads = queries.reshape(local_rows, KVH, group_size, HD)
    past_keys = cache_keys.reshape(local_rows, cache_span, KVH, HD)
    past_values = cache_values.reshape(local_rows, cache_span, KVH, HD)
    score_scale = 1.0 / math.sqrt(HD)
    past_scores = (
        jnp.einsum("tgqd,tcgd->tgqc", query_heads, past_keys, preferred_element_type=jnp.float32)
        * score_scale
    )
    own_scores = (
        jnp.einsum(
            "tgqd,tgd->tgq",
            query_heads,
            new_keys.reshape(local_rows, KVH, HD),
            preferred_element_type=jnp.float32,
        )
        * score_scale
    )
    is_valid = lax.broadcasted_iota(jnp.int32, (local_rows, cache_span), 1) < cache_len[:, None]
    past_scores = jnp.where(is_valid[:, None, None, :], past_scores, -1e30)
    peak_score = jnp.maximum(jnp.max(past_scores, axis=3), own_scores)
    past_exp = jnp.exp(past_scores - peak_score[..., None])
    own_exp = jnp.exp(own_scores - peak_score)
    denom_sum = jnp.sum(past_exp, axis=3) + own_exp
    past_weights = (past_exp / denom_sum[..., None]).astype(jnp.bfloat16)
    own_weights = (own_exp / denom_sum).astype(jnp.bfloat16)
    blended = jnp.einsum(
        "tgqc,tcgd->tgqd", past_weights, past_values, preferred_element_type=jnp.float32
    )
    blended = blended + own_weights.astype(jnp.float32)[..., None] * new_values.reshape(
        local_rows, KVH, 1, HD
    ).astype(jnp.float32)
    return blended.reshape(local_rows, H * HD).astype(jnp.bfloat16)


MESH = pl.DeviceIdType.MESH
VMEM_LIMIT = 66_000_000


class Place:
    def __init__(self, side, depth):
        self.side, self.depth = side, depth
        ep = lax.axis_index("ep")
        self.ep = ep
        self.core = lax.rem(ep, 2)
        self.x = lax.rem(ep // 2, side)
        self.y = ep // (2 * side)
        self.z = lax.axis_index("dp")

    def at(self, dy=0, dx=0, dz=0, flip=False):
        y, x = self.line(dy, dx)
        z = lax.rem(self.z + dz, self.depth) if dz else self.z
        core = 1 - self.core if flip else self.core
        return ((y * self.side + x) * 2 + core, z)

    def line(self, dy, dx):
        return lax.rem(self.y + dy, self.side), lax.rem(self.x + dx, self.side)


def greet(devices):
    barrier = pltpu.get_barrier_semaphore()
    for device in devices:
        pl.semaphore_signal(barrier, inc=1, device_id=device, device_id_type=MESH)
    pl.semaphore_wait(barrier, len(devices))


def remote(src, dst, send, recv, device):
    return pltpu.make_async_remote_copy(
        src_ref=src, dst_ref=dst, send_sem=send, recv_sem=recv, device_id=device, device_id_type=MESH
    )


def slices_of(width, extra=0):
    step = 512
    cuts = [[start, step] for start in range(0, width, step)]
    cuts[-1][1] += extra
    return cuts


def reduce_shapes(side, depth, rows, width):
    n = width // 512
    lines = side * side
    bf, dma = jnp.bfloat16, pltpu.SemaphoreType.DMA
    tall = depth * rows
    return [
        pltpu.VMEM((side, side, tall, width), bf),
        pltpu.VMEM((side - 1, side, tall, width), bf),
        pltpu.VMEM((side, tall, width), bf),
        pltpu.VMEM((side - 1, tall, width), bf),
        pltpu.VMEM((depth, rows, width), bf),
        pltpu.VMEM((max(depth - 1, 1), rows, width), bf),
        dma((n, 2)),
        dma((n, side, side, 2)),
        dma((n, side, 2)),
        dma((n, depth, 2)),
    ]


def reduce_scatter(here, rows, width, produce, finish, lags, part, scratch):
    in1, in2, sum2, in3, sum3, in4, sem1, sem2, sem3, sem4 = scratch
    side, depth = here.side, here.depth
    cuts = slices_of(width)
    sends = []

    def core_copy(s):
        start, size = cuts[s]
        cols = pl.ds(start, size)
        return remote(
            part.at[:, :, 1 - here.core, :, cols],
            in1.at[:, :, :, cols],
            sem1.at[s, 0],
            sem1.at[s, 1],
            here.at(flip=True),
        )

    def offsets(s, a, b):
        return (a, b) if s % 2 == 0 else (b, a)

    def first_copy(s, ja, kb, sending):
        cols = pl.ds(*cuts[s])
        slot = side - ja - 1
        y, x = here.line(*offsets(s, ja, kb))
        return remote(
            in1.at[y, x, :, cols],
            in2.at[slot, kb, :, cols],
            sem2.at[s, ja, kb, 0],
            sem2.at[s, side - ja if sending else ja, kb, 1],
            here.at(*offsets(s, ja, 0)),
        )

    def second_copy(s, kb, sending):
        cols = pl.ds(*cuts[s])
        return remote(
            sum2.at[kb, :, cols],
            in3.at[side - kb - 1, :, cols],
            sem3.at[s, kb, 0],
            sem3.at[s, side - kb if sending else kb, 1],
            here.at(*offsets(s, 0, kb)),
        )

    def depth_copy(s, jz, sending):
        cols = pl.ds(*cuts[s])
        return remote(
            sum3.at[lax.rem(here.z + jz, depth), :, cols],
            in4.at[depth - jz - 1, :, cols],
            sem4.at[s, jz, 0],
            sem4.at[s, depth - jz if sending else jz, 1],
            here.at(0, 0, jz),
        )

    def go(copy):
        copy.start()
        sends.append(copy)

    def wide(value):
        return value.astype(jnp.float32)

    def phase0(s):
        cols = pl.ds(*cuts[s])
        value = produce(s, cols)
        part[:, :, :, :, cols] = value.astype(jnp.bfloat16).reshape(
            side, side, 2, depth * rows, cuts[s][1]
        )
        go(core_copy(s))

    def phase1(s):
        cols = pl.ds(*cuts[s])
        core_copy(s).wait_recv()
        for a in list(range(1, side)) + [0]:
            for b in list(range(1, side)) + [0]:
                y, x = here.line(*offsets(s, a, b))
                total = wide(part[y, x, here.core, :, cols]) + wide(in1[y, x, :, cols])
                in1[y, x, :, cols] = total.astype(jnp.bfloat16)
                if a:
                    go(first_copy(s, a, b, True))

    def phase2(s):
        cols = pl.ds(*cuts[s])
        for b in list(range(1, side)) + [0]:
            y, x = here.line(*offsets(s, 0, b))
            total = wide(in1[y, x, :, cols])
            for a in range(1, side):
                first_copy(s, a, b, False).wait_recv()
                total = total + wide(in2[a - 1, b, :, cols])
            sum2[b, :, cols] = total.astype(jnp.bfloat16)
            if b:
                go(second_copy(s, b, True))

    def phase3(s):
        cols = pl.ds(*cuts[s])
        total = wide(sum2[0, :, cols])
        for b in range(1, side):
            second_copy(s, b, False).wait_recv()
            total = total + wide(in3[b - 1, :, cols])
        if depth == 1:
            finish(s, cols, total)
            return
        sum3[:, :, cols] = total.astype(jnp.bfloat16).reshape(depth, rows, cuts[s][1])
        for jz in range(1, depth):
            go(depth_copy(s, jz, True))

    def phase4(s):
        if depth == 1:
            return
        cols = pl.ds(*cuts[s])
        total = wide(sum3[here.z, :, cols])
        for jz in range(1, depth):
            depth_copy(s, jz, False).wait_recv()
            total = total + wide(in4[jz - 1, :, cols])
        finish(s, cols, total)

    phases = tuple(zip((phase0, phase1, phase2, phase3, phase4), lags))
    for step in range(len(cuts) + phases[-1][1]):
        for phase, lag in phases:
            if 0 <= step - lag < len(cuts):
                phase(step - lag)
    for copy in sends:
        copy.wait_send()


def plane_of(here):
    side = here.side
    return (
        [here.at(flip=True)]
        + [here.at(dy=j) for j in range(1, side)]
        + [here.at(dx=j) for j in range(1, side)]
    )


def projection_kernel(
    side, attended, weight_hbm, resid, gain, router, chosen, hidden, packed, weight, regrouped, part, wsem, ssem, rsem, *scratch
):
    here = Place(side, 1)
    rows = attended.shape[0]
    count = 2 * side * side
    width = attended.shape[1] // count
    z = lax.axis_index("dp")
    load = pltpu.make_async_copy(weight_hbm, weight, wsem)
    load.start()

    def peer(j):
        return lax.rem(here.ep + j, count)

    greet([(peer(j), z) for j in range(1, count)])

    def piece(index):
        return attended.at[:, pl.ds(pl.multiple_of(index * width, 128), width)]

    def exchange(j, sending):
        return remote(
            piece(peer(j)),
            regrouped.at[here.ep],
            ssem.at[j],
            rsem.at[count - j if sending else j],
            (peer(j), z),
        )

    for j in range(1, count):
        exchange(j, True).start()
    regrouped[here.ep] = attended[:, pl.ds(pl.multiple_of(here.ep * width, 128), width)]
    load.wait()
    for j in range(1, count):
        remote(
            piece(peer(j)), regrouped.at[peer(j)], ssem.at[j], rsem.at[j], (peer(j), z)
        ).wait_recv()

    def produce(s, cols):
        left = regrouped[...].reshape(count * rows, width)
        return jnp.dot(left, weight[:, cols], preferred_element_type=jnp.float32)

    def finish(s, cols, total):
        value = resid[:, cols].astype(jnp.float32) + total
        hidden[:, cols] = value
        squares.append(jnp.sum(value * value, axis=1, keepdims=True))

    squares = []

    reduce_scatter(here, rows, hidden.shape[1], produce, finish, (0, 2, 5, 8, 8), part, scratch)
    features = hidden.shape[1]
    scale = lax.rsqrt(jnp.maximum(sum(squares) / features, 0.25))
    logits = jnp.zeros((rows, router.shape[1]), jnp.float32)
    for start, size in slices_of(features):
        cols = pl.ds(start, size)
        normed = (hidden[:, cols] * scale * gain[:, cols]).astype(jnp.bfloat16)
        packed[:, cols] = normed
        logits = logits + jnp.dot(normed, router[cols, :], preferred_element_type=jnp.float32)
    named = chosen[...] > 0
    peak = jnp.max(jnp.where(named, logits, -jnp.inf), axis=1, keepdims=True)
    grown = jnp.where(named, jnp.exp(jnp.where(named, logits - peak, 0.0)), 0.0)
    probs = grown / jnp.sum(grown, axis=1, keepdims=True)
    packed[:, features:] = jnp.zeros((rows, packed.shape[1] - features), jnp.bfloat16)
    packed[:, features : features + router.shape[1]] = probs.astype(jnp.bfloat16)
    for j in range(1, count):
        exchange(j, True).wait_send()


def project(side, attended, out_proj, resid, gain, router, chosen):
    rows, width = resid.shape
    count = 2 * side * side
    dma = pltpu.SemaphoreType.DMA
    vmem = pl.BlockSpec(memory_space=pltpu.VMEM)
    return pl.pallas_call(
        lambda *refs: projection_kernel(side, *refs),
        out_shape=(
            jax.ShapeDtypeStruct((rows, width), jnp.float32),
            jax.ShapeDtypeStruct((rows, width + pl.cdiv(router.shape[1], 128) * 128), jnp.bfloat16),
        ),
        in_specs=[vmem, pl.BlockSpec(memory_space=pl.ANY), vmem, vmem, vmem, vmem],
        out_specs=(vmem, vmem),
        scratch_shapes=[
            pltpu.VMEM(out_proj.shape, jnp.bfloat16),
            pltpu.VMEM((count, rows, attended.shape[1] // count), jnp.bfloat16),
            pltpu.VMEM((side, side, 2, rows, width), jnp.bfloat16),
            dma(()),
            dma((count,)),
            dma((count,)),
        ]
        + reduce_shapes(side, 1, rows, width),
        compiler_params=pltpu.CompilerParams(
            collective_id=0, has_side_effects=True, vmem_limit_bytes=VMEM_LIMIT
        ),
    )(attended, out_proj, resid, gain, router, chosen)


AXES = ("y", "x", "z")
ORDERS = (
    ("y", "x", "z"),
    ("z", "x", "y"),
    ("y", "z", "x"),
    ("y", "x", "z"),
    ("z", "x", "y"),
    ("y", "z", "x"),
    ("y", "x", "z"),
    ("z", "x", "y"),
)
STEP = 512
HALF = 256


class Spot:
    def __init__(self):
        ep = lax.axis_index("ep")
        self.core = lax.rem(ep, 2)
        self.pos = {"x": lax.rem(ep // 2, 4), "y": ep // 8, "z": lax.axis_index("dp")}

    def coord(self, axis, off):
        return lax.rem(self.pos[axis] + off, 4) if off else self.pos[axis]

    def at(self, axis=None, off=0, flip=False):
        place = dict(self.pos)
        if axis:
            place[axis] = self.coord(axis, off)
        core = 1 - self.core if flip else self.core
        return ((place["y"] * 4 + place["x"]) * 2 + core, place["z"])

    def index(self, fixed):
        return tuple(fixed.get(axis, slice(None)) for axis in AXES)


def expert_kernel(own, gate_hbm, up_hbm, down_hbm, mixed, *scratch):
    n = len(ORDERS)
    gu, down, act, total, wsem, nsem, fsem, csem, rnear, rfar, rcore = scratch[:11]
    scratch = scratch[11:]
    held, inner = scratch[:n], scratch[n : 2 * n]
    nears = [scratch[2 * n + 3 * s : 2 * n + 3 * s + 3] for s in range(n)]
    fars = [scratch[5 * n + 3 * s : 5 * n + 3 * s + 3] for s in range(n)]
    here = Spot()
    rows = own.shape[0]
    hidden = act.shape[1]
    loads = [
        pltpu.make_async_copy(gate_hbm.at[0], gu.at[:, pl.ds(0, hidden)], wsem.at[0]),
        pltpu.make_async_copy(up_hbm.at[0], gu.at[:, pl.ds(hidden, hidden)], wsem.at[1]),
        pltpu.make_async_copy(down_hbm.at[0], down, wsem.at[2]),
    ]
    for load in loads:
        load.start()
    greet([here.at(flip=True)] + [here.at(axis, off) for axis in AXES for off in (1, 2, 3)])
    sends = []

    def go(copy):
        copy.start()
        sends.append(copy)

    def cols_of(s):
        return pl.ds(STEP * s, held[s].shape[-1])

    def halves(s, d, width):
        return (slice(None),) * 1 + (pl.ds(0, HALF) if d == 0 else pl.ds(HALF, width - HALF),)

    def spread_index(s, p, off, core=None):
        order = ORDERS[s]
        fixed = {axis: here.pos[axis] for axis in order[p + 1 :]}
        fixed[order[p]] = here.coord(order[p], off)
        return (here.core if core is None else core,) + here.index(fixed)

    def spread(s, p, off, core=None):
        return held[s].at[spread_index(s, p, off, core)]

    def spread_half(s, p, off, d):
        width = held[s].shape[-1]
        return held[s].at[spread_index(s, p, off) + halves(s, d, width)]

    def direct_gather(s, p):
        return p == 0 or (p == 1 and s < 3)

    def gather_near(s, p):
        axis = ORDERS[s][p]
        for d, off in enumerate((1, 3)):
            src = own.at[:, cols_of(s)] if p == 0 else spread(s, p, 0)
            go(remote(src, spread(s, p, 0), nsem.at[s, p, d, 0], nsem.at[s, p, d, 1], here.at(axis, off)))
        if direct_gather(s, p):
            src = own.at[:, cols_of(s)] if p == 0 else spread(s, p, 0)
            go(remote(src, spread(s, p, 0), fsem.at[s, p, 0, 0], fsem.at[s, p, 0, 1], here.at(axis, 2)))
        if p == 2:
            give(s, 0, 0)

    def gather_far(s, p):
        axis = ORDERS[s][p]
        for d, (off, back) in enumerate(((1, 3), (3, 1))):
            ref = spread(s, p, back)
            remote(ref, ref, nsem.at[s, p, d, 0], nsem.at[s, p, d, 1], here.at(axis, back)).wait_recv()
            if not direct_gather(s, p):
                ref = spread_half(s, p, back, d)
                go(remote(ref, ref, fsem.at[s, p, d, 0], fsem.at[s, p, d, 1], here.at(axis, off)))
            if p == 2:
                give(s, 1 + d, back)

    def gather_end(s, p):
        axis = ORDERS[s][p]
        if direct_gather(s, p):
            ref = spread(s, p, 2)
            remote(ref, ref, fsem.at[s, p, 0, 0], fsem.at[s, p, 0, 1], here.at(axis, 2)).wait_recv()
        else:
            for d, back in enumerate((3, 1)):
                ref = spread_half(s, p, 2, d)
                remote(ref, ref, fsem.at[s, p, d, 0], fsem.at[s, p, d, 1], here.at(axis, back)).wait_recv()
        if p == 2:
            give(s, 3, 2)

    def give(s, k, off):
        ref = spread(s, 2, off)
        go(remote(ref, ref, csem.at[s, k, 0], csem.at[s, k, 1], here.at(flip=True)))

    def take(s):
        for k, off in enumerate((0, 3, 1, 2)):
            ref = spread(s, 2, off, 1 - here.core)
            remote(ref, ref, csem.at[s, k, 0], csem.at[s, k, 1], here.at(flip=True)).wait_recv()

    group = 32 * rows

    def rows_at(i):
        return pl.ds(pl.multiple_of(i * group, group), group)

    def consume(s):
        if s == 0:
            loads[0].wait()
            loads[1].wait()

        def step(i, carry):
            block = held[s][i // 2, pl.ds(2 * lax.rem(i, 2), 2), :, :, :, :STEP].reshape(group, STEP)
            value = jnp.dot(block, gu[STEP * s : STEP * s + STEP, :], preferred_element_type=jnp.float32)
            total[rows_at(i), :] = value if s == 0 else total[rows_at(i), :] + value
            return carry

        lax.fori_loop(0, 4, step, 0)

    def start(s):
        held[s][here.core, here.pos["y"], here.pos["x"], here.pos["z"]] = own[:, cols_of(s)]
        gather_near(s, 0)

    def second(s):
        gather_far(s, 0)
        gather_end(s, 0)
        gather_near(s, 1)

    def third(s):
        gather_far(s, 1)

    def fourth(s):
        gather_end(s, 1)
        gather_near(s, 2)

    def fifth(s):
        gather_far(s, 2)

    def sixth(s):
        gather_end(s, 2)
        take(s)
        consume(s)

    groups = ((0, 1, 2), (3, 4, 5), (6, 7))
    plan = (
        (start, 0), (start, 1), (start, 2),
        (second, 0), (second, 1), (third, 0), (second, 2), (fourth, 0),
        (third, 1), (fourth, 1), (third, 2), (fifth, 0), (fourth, 2),
        (sixth, 0), (fifth, 1), (sixth, 1), (fifth, 2), (sixth, 2),
    )
    for phase, g in plan:
        for s in groups[g]:
            phase(s)
    for copy in sends:
        copy.wait_send()
    sends.clear()
    loads[2].wait()
    expert = (lax.axis_index("ep") * 4 + here.pos["z"]) // 2

    def activate(i, carry):
        tail = held[n - 1][i // 2, pl.ds(2 * lax.rem(i, 2), 2), :, :, :, STEP:].reshape(group, 128)
        lane = lax.broadcasted_iota(jnp.int32, tail.shape, 1)
        weight = jnp.sum(jnp.where(lane == expert, tail.astype(jnp.float32), 0.0), axis=1, keepdims=True)
        gate_val = total[rows_at(i), :hidden]
        value = gate_val / (1.0 + jnp.exp(-gate_val)) * total[rows_at(i), hidden:] * weight
        act[rows_at(i), :] = value.astype(jnp.bfloat16)
        return carry

    lax.fori_loop(0, 4, activate, 0)

    def fold(s, p, off):
        order = ORDERS[s][::-1]
        fixed = {axis: here.pos[axis] for axis in order[:p]}
        fixed[order[p]] = here.coord(order[p], off)
        return here.index(fixed)

    def direct_fold(s, p):
        return p == 2 or (p == 1 and s >= n - 2)

    def gain(s, p, off):
        index = fold(s, p, off)
        if p == 0:
            mine = held[s][(here.core,) + index + (slice(None), pl.ds(0, STEP))]
            return mine + inner[s][index]
        return inner[s][index]

    def core_copy(s):
        return remote(
            held[s].at[1 - here.core, :, :, :, :, pl.ds(0, STEP)],
            inner[s],
            rcore.at[s, 0],
            rcore.at[s, 1],
            here.at(flip=True),
        )

    def produce(s):
        def step(core):
            def one(h, carry):
                i = 2 * core + h
                value = jnp.dot(
                    act[rows_at(i), :], down[:, STEP * s : STEP * s + STEP], preferred_element_type=jnp.float32
                )
                held[s][core, pl.ds(2 * h, 2), :, :, :, :STEP] = value.astype(jnp.bfloat16).reshape(
                    2, 4, 4, rows, STEP
                )
                return carry

            lax.fori_loop(0, 2, one, 0)

        step(1 - here.core)
        go(core_copy(s))
        step(here.core)

    def half_of(ref, index, d):
        return ref.at[index + (slice(None), pl.ds(HALF * d, HALF))]

    def lead(p):
        return (slice(None),) * (2 - p)

    def far_copy(s, p, d, sending):
        axis = ORDERS[s][2 - p]
        index = fold(s, p, 2)
        if direct_fold(s, p):
            return remote(
                inner[s].at[index], fars[s][p], rfar.at[s, p, 0, 0], rfar.at[s, p, 0, 1], here.at(axis, 2)
            )
        return remote(
            half_of(inner[s], index, d),
            half_of(fars[s][p], lead(p), d),
            rfar.at[s, p, d, 0],
            rfar.at[s, p, d, 1],
            here.at(axis, (1, 3)[d]),
        )

    def near_copy(s, p, d):
        axis = ORDERS[s][2 - p]
        off = (1, 3)[d]
        return remote(
            inner[s].at[fold(s, p, off)],
            nears[s][p].at[d],
            rnear.at[s, p, d, 0],
            rnear.at[s, p, d, 1],
            here.at(axis, off),
        )

    def fold_far(s, p):
        if p == 0:
            core_copy(s).wait_recv()
            inner[s][fold(s, 0, 2)] = gain(s, 0, 2)
        if direct_fold(s, p):
            go(far_copy(s, p, 0, True))
            fold_near(s, p)
        else:
            for d in range(2):
                go(far_copy(s, p, d, True))

    def fold_near(s, p):
        for d, off in enumerate((1, 3)):
            index = fold(s, p, off)
            if direct_fold(s, p):
                if p == 0:
                    inner[s][index] = gain(s, p, off)
            else:
                far_copy(s, p, d, False).wait_recv()
                if p == 0:
                    inner[s][index] = gain(s, p, off)
                part = index + (slice(None), pl.ds(HALF * d, HALF))
                inner[s][part] = inner[s][part] + fars[s][p][lead(p) + (slice(None), pl.ds(HALF * d, HALF))]
            go(near_copy(s, p, d))

    def fold_end(s, p):
        value = gain(s, p, 0).astype(jnp.float32)
        for d in range(2):
            near_copy(s, p, d).wait_recv()
            value = value + nears[s][p][d].astype(jnp.float32)
        if direct_fold(s, p):
            far_copy(s, p, 0, False).wait_recv()
            value = value + fars[s][p][...].astype(jnp.float32)
        if p == 2:
            mixed[:, STEP * s : STEP * s + STEP] = value
        else:
            inner[s][fold(s, p, 0)] = value.astype(jnp.bfloat16)

    def next_fold(s, p):
        fold_end(s, p - 1)
        fold_far(s, p)

    def middle(s):
        if not direct_fold(s, 1):
            fold_near(s, 1)

    phases = (
        (produce, 0),
        (lambda s: fold_far(s, 0), 1),
        (lambda s: fold_near(s, 0), 3),
        (lambda s: next_fold(s, 1), 5),
        (middle, 6),
        (lambda s: next_fold(s, 2), 7),
        (lambda s: fold_end(s, 2), 8),
    )
    for step in range(n + phases[-1][1]):
        for phase, lag in phases:
            if 0 <= step - lag < n:
                phase(step - lag)
    for copy in sends:
        copy.wait_send()


def run_experts(packed, gate_slab, up_slab, down_slab):
    rows, width = packed.shape[0], down_slab.shape[2]
    hidden = gate_slab.shape[2]
    n = len(ORDERS)
    dma, bf = pltpu.SemaphoreType.DMA, jnp.bfloat16
    vmem, anywhere = pl.BlockSpec(memory_space=pltpu.VMEM), pl.BlockSpec(memory_space=pl.ANY)
    widths = [STEP] * (n - 1) + [STEP + packed.shape[1] - width]
    shapes = [
        pltpu.VMEM((gate_slab.shape[1], 2 * hidden), bf),
        pltpu.VMEM(down_slab.shape[1:], bf),
        pltpu.VMEM((128 * rows, hidden), bf),
        pltpu.VMEM((128 * rows, 2 * hidden), jnp.float32),
        dma((3,)),
        dma((n, 3, 2, 2)),
        dma((n, 3, 2, 2)),
        dma((n, 4, 2)),
        dma((n, 3, 2, 2)),
        dma((n, 3, 2, 2)),
        dma((n, 2)),
    ]
    shapes += [pltpu.VMEM((2, 4, 4, 4, rows, w), bf) for w in widths]
    shapes += [pltpu.VMEM((4, 4, 4, rows, STEP), bf)] * n
    shapes += [pltpu.VMEM((2,) + (4,) * (2 - p) + (rows, STEP), bf) for _ in range(n) for p in range(3)]
    shapes += [pltpu.VMEM((4,) * (2 - p) + (rows, STEP), bf) for _ in range(n) for p in range(3)]
    return pl.pallas_call(
        expert_kernel,
        out_shape=jax.ShapeDtypeStruct((rows, width), jnp.float32),
        in_specs=[vmem, anywhere, anywhere, anywhere],
        out_specs=vmem,
        scratch_shapes=shapes,
        compiler_params=pltpu.CompilerParams(
            collective_id=1, has_side_effects=True, vmem_limit_bytes=VMEM_LIMIT
        ),
    )(packed, gate_slab, up_slab, down_slab)


def local(
    resid,
    queries,
    new_keys,
    new_values,
    cache_keys,
    cache_values,
    cache_len,
    out_proj,
    norm_gain,
    router,
    expert_ids,
    gate_slab,
    up_slab,
    down_slab,
):
    attended = attend(queries, new_keys, new_values, cache_keys, cache_values, cache_len)
    side = math.isqrt(lax.axis_size("ep") // 2)
    labels = jnp.arange(router.shape[1], dtype=jnp.int32)
    chosen = jnp.any(expert_ids[:, :, None] == labels[None, None, :], axis=1).astype(jnp.float32)
    hidden, packed = project(
        side, attended, out_proj, resid, norm_gain.reshape(1, -1), router, chosen
    )
    return hidden + run_experts(packed, gate_slab, up_slab, down_slab)


def solution(mesh):
    in_specs = (
        P(("ep", "dp"), None),
        P(("ep", "dp"), None),
        P(("ep", "dp"), None),
        P(("ep", "dp"), None),
        P(("ep", "dp"), None, None),
        P(("ep", "dp"), None, None),
        P(("ep", "dp")),
        P("ep", None),
        P(),
        P(),
        P(("ep", "dp"), None),
        P(("ep", "dp"), None, None),
        P(("ep", "dp"), None, None),
        P(("ep", "dp"), None, None),
    )
    out_specs = P(("ep", "dp"), None)
    return jax.shard_map(local, mesh=mesh, in_specs=in_specs, out_specs=out_specs, check_vma=False)
```

```python
import math

import jax
import jax.numpy as jnp
from jax import lax
from jax.experimental import pallas as pl
from jax.experimental.pallas import tpu as pltpu
from jax.sharding import PartitionSpec as P

D = 4096
H = 64
KVH = 4
HD = 128
TOP = 8


MESH = pl.DeviceIdType.MESH
VMEM_LIMIT = 66_000_000


class Place:
    def __init__(self, side, depth):
        self.side, self.depth = side, depth
        ep = lax.axis_index("ep")
        self.ep = ep
        self.core = lax.rem(ep, 2)
        self.x = lax.rem(ep // 2, side)
        self.y = ep // (2 * side)
        self.z = lax.axis_index("dp")

    def at(self, dy=0, dx=0, dz=0, flip=False):
        y, x = self.line(dy, dx)
        z = lax.rem(self.z + dz, self.depth) if dz else self.z
        core = 1 - self.core if flip else self.core
        return ((y * self.side + x) * 2 + core, z)

    def line(self, dy, dx):
        return lax.rem(self.y + dy, self.side), lax.rem(self.x + dx, self.side)


def greet(devices):
    barrier = pltpu.get_barrier_semaphore()
    for device in devices:
        pl.semaphore_signal(barrier, inc=1, device_id=device, device_id_type=MESH)
    pl.semaphore_wait(barrier, len(devices))


def remote(src, dst, send, recv, device):
    return pltpu.make_async_remote_copy(
        src_ref=src, dst_ref=dst, send_sem=send, recv_sem=recv, device_id=device, device_id_type=MESH
    )


def slices_of(width, extra=0):
    step = 512
    cuts = [[start, step] for start in range(0, width, step)]
    cuts[-1][1] += extra
    return cuts


def reduce_shapes(side, depth, rows, width):
    n = width // 512
    lines = side * side
    bf, dma = jnp.bfloat16, pltpu.SemaphoreType.DMA
    tall = depth * rows
    return [
        pltpu.VMEM((side, side, tall, width), bf),
        pltpu.VMEM((side - 1, side, tall, width), bf),
        pltpu.VMEM((side, tall, width), bf),
        pltpu.VMEM((side - 1, tall, width), bf),
        pltpu.VMEM((depth, rows, width), bf),
        pltpu.VMEM((max(depth - 1, 1), rows, width), bf),
        dma((n, 2)),
        dma((n, side, side, 2)),
        dma((n, side, 2)),
        dma((n, depth, 2)),
    ]


def reduce_scatter(here, rows, width, produce, finish, lags, part, scratch):
    in1, in2, sum2, in3, sum3, in4, sem1, sem2, sem3, sem4 = scratch
    side, depth = here.side, here.depth
    cuts = slices_of(width)
    sends = []

    def core_copy(s):
        start, size = cuts[s]
        cols = pl.ds(start, size)
        return remote(
            part.at[:, :, 1 - here.core, :, cols],
            in1.at[:, :, :, cols],
            sem1.at[s, 0],
            sem1.at[s, 1],
            here.at(flip=True),
        )

    def offsets(s, a, b):
        return (a, b) if s % 2 == 0 else (b, a)

    def first_copy(s, ja, kb, sending):
        cols = pl.ds(*cuts[s])
        slot = side - ja - 1
        y, x = here.line(*offsets(s, ja, kb))
        return remote(
            in1.at[y, x, :, cols],
            in2.at[slot, kb, :, cols],
            sem2.at[s, ja, kb, 0],
            sem2.at[s, side - ja if sending else ja, kb, 1],
            here.at(*offsets(s, ja, 0)),
        )

    def second_copy(s, kb, sending):
        cols = pl.ds(*cuts[s])
        return remote(
            sum2.at[kb, :, cols],
            in3.at[side - kb - 1, :, cols],
            sem3.at[s, kb, 0],
            sem3.at[s, side - kb if sending else kb, 1],
            here.at(*offsets(s, 0, kb)),
        )

    def depth_copy(s, jz, sending):
        cols = pl.ds(*cuts[s])
        return remote(
            sum3.at[lax.rem(here.z + jz, depth), :, cols],
            in4.at[depth - jz - 1, :, cols],
            sem4.at[s, jz, 0],
            sem4.at[s, depth - jz if sending else jz, 1],
            here.at(0, 0, jz),
        )

    def go(copy):
        copy.start()
        sends.append(copy)

    def wide(value):
        return value.astype(jnp.float32)

    def phase0(s):
        cols = pl.ds(*cuts[s])
        value = produce(s, cols)
        part[:, :, :, :, cols] = value.astype(jnp.bfloat16).reshape(
            side, side, 2, depth * rows, cuts[s][1]
        )
        go(core_copy(s))

    def phase1(s):
        cols = pl.ds(*cuts[s])
        core_copy(s).wait_recv()
        for a in list(range(1, side)) + [0]:
            for b in list(range(1, side)) + [0]:
                y, x = here.line(*offsets(s, a, b))
                total = wide(part[y, x, here.core, :, cols]) + wide(in1[y, x, :, cols])
                in1[y, x, :, cols] = total.astype(jnp.bfloat16)
                if a:
                    go(first_copy(s, a, b, True))

    def phase2(s):
        cols = pl.ds(*cuts[s])
        for b in list(range(1, side)) + [0]:
            y, x = here.line(*offsets(s, 0, b))
            total = wide(in1[y, x, :, cols])
            for a in range(1, side):
                first_copy(s, a, b, False).wait_recv()
                total = total + wide(in2[a - 1, b, :, cols])
            sum2[b, :, cols] = total.astype(jnp.bfloat16)
            if b:
                go(second_copy(s, b, True))

    def phase3(s):
        cols = pl.ds(*cuts[s])
        total = wide(sum2[0, :, cols])
        for b in range(1, side):
            second_copy(s, b, False).wait_recv()
            total = total + wide(in3[b - 1, :, cols])
        if depth == 1:
            finish(s, cols, total)
            return
        sum3[:, :, cols] = total.astype(jnp.bfloat16).reshape(depth, rows, cuts[s][1])
        for jz in range(1, depth):
            go(depth_copy(s, jz, True))

    def phase4(s):
        if depth == 1:
            return
        cols = pl.ds(*cuts[s])
        total = wide(sum3[here.z, :, cols])
        for jz in range(1, depth):
            depth_copy(s, jz, False).wait_recv()
            total = total + wide(in4[jz - 1, :, cols])
        finish(s, cols, total)

    phases = tuple(zip((phase0, phase1, phase2, phase3, phase4), lags))
    for step in range(len(cuts) + phases[-1][1]):
        for phase, lag in phases:
            if 0 <= step - lag < len(cuts):
                phase(step - lag)
    for copy in sends:
        copy.wait_send()


def plane_of(here):
    side = here.side
    return (
        [here.at(flip=True)]
        + [here.at(dy=j) for j in range(1, side)]
        + [here.at(dx=j) for j in range(1, side)]
    )


def attend(queries, new_keys, new_values, keys, values, lengths, attended, qs, os, nk, nv):
    tokens = queries.shape[0]
    share = H // KVH
    scale = 1.0 / math.sqrt(HD)
    for h in range(H):
        qs[tokens * h : tokens * h + tokens, :] = queries[:, HD * h : HD * h + HD].astype(jnp.float32)
    nk[...] = new_keys[...].astype(jnp.float32)
    nv[...] = new_values[...].astype(jnp.float32)

    def spread(row):
        return jnp.concatenate(
            [jnp.broadcast_to(row[:, HD * g : HD * g + HD], (share, HD)) for g in range(KVH)], axis=0
        )

    def one(t):
        rows = pl.ds(t, H, stride=tokens)
        query = qs[rows, :]
        narrow = query.astype(jnp.bfloat16)
        scores = jnp.concatenate(
            [
                lax.dot_general(
                    narrow[share * g : share * g + share],
                    keys[t, :, HD * g : HD * g + HD],
                    (((1,), (1,)), ((), ())),
                    preferred_element_type=jnp.float32,
                )
                for g in range(KVH)
            ],
            axis=0,
        )
        own = jnp.sum(query * spread(nk[pl.ds(t, 1), :]), axis=1, keepdims=True) * scale
        valid = lax.broadcasted_iota(jnp.int32, scores.shape, 1) < lengths[t]
        scores = jnp.where(valid, scores * scale, -1e30)
        peak = jnp.maximum(jnp.max(scores, axis=1, keepdims=True), own)
        grown = jnp.exp(scores - peak)
        own_grown = jnp.exp(own - peak)
        denom = jnp.sum(grown, axis=1, keepdims=True) + own_grown
        weights = (grown / denom).astype(jnp.bfloat16)
        own_weight = (own_grown / denom).astype(jnp.bfloat16).astype(jnp.float32)
        blended = jnp.concatenate(
            [
                jnp.dot(
                    weights[share * g : share * g + share],
                    values[t, :, HD * g : HD * g + HD],
                    preferred_element_type=jnp.float32,
                )
                for g in range(KVH)
            ],
            axis=0,
        )
        os[rows, :] = blended + own_weight * spread(nv[pl.ds(t, 1), :])

    def several(i, carry):
        for k in range(4):
            one(4 * i + k)
        return carry

    lax.fori_loop(0, tokens // 4, several, 0)
    attended[...] = os[...].astype(jnp.bfloat16).reshape(attended.shape)


def projection_kernel(
    side, queries, new_keys, new_values, keys_hbm, values_hbm, lengths, weight_hbm, resid, gain, router, ids,
    hidden, packed, attended, keys, values, qs, os, nk, nv, weight, regrouped, part, wsem, ssem, rsem, *scratch
):
    here = Place(side, 1)
    rows = queries.shape[0]
    count = 2 * side * side
    z = lax.axis_index("dp")
    caches = [
        pltpu.make_async_copy(keys_hbm, keys, wsem.at[1]),
        pltpu.make_async_copy(values_hbm, values, wsem.at[2]),
    ]
    load = pltpu.make_async_copy(weight_hbm, weight, wsem.at[0])
    for copy in caches:
        copy.start()
    load.start()

    def peer(j):
        return lax.rem(here.ep + j, count)

    barrier = pltpu.get_barrier_semaphore()
    for j in range(1, count):
        pl.semaphore_signal(barrier, inc=1, device_id=(peer(j), z), device_id_type=MESH)
    for copy in caches:
        copy.wait()
    attend(queries, new_keys, new_values, keys, values, lengths, attended, qs, os, nk, nv)
    pl.semaphore_wait(barrier, count - 1)

    def exchange(j, sending):
        return remote(
            attended.at[peer(j)],
            regrouped.at[here.ep],
            ssem.at[j],
            rsem.at[count - j if sending else j],
            (peer(j), z),
        )

    for j in range(1, count):
        exchange(j, True).start()
    regrouped[here.ep] = attended[here.ep]
    load.wait()
    for j in range(1, count):
        remote(
            attended.at[peer(j)], regrouped.at[peer(j)], ssem.at[j], rsem.at[j], (peer(j), z)
        ).wait_recv()

    def produce(s, cols):
        left = jnp.concatenate([regrouped[:, k].reshape(count * rows, HD) for k in range(2)], axis=1)
        return jnp.dot(left, weight[:, cols], preferred_element_type=jnp.float32)

    def finish(s, cols, total):
        value = resid[:, cols].astype(jnp.float32) + total
        hidden[:, cols] = value
        squares.append(jnp.sum(value * value, axis=1, keepdims=True))

    squares = []

    reduce_scatter(here, rows, hidden.shape[1], produce, finish, (0, 2, 5, 8, 8), part, scratch)
    features = hidden.shape[1]
    scale = lax.rsqrt(jnp.maximum(sum(squares) / features, 0.25))
    experts = router.shape[0]
    logits = jnp.zeros((rows, experts), jnp.float32)
    last_dims = (((1,), (1,)), ((), ()))
    for start, size in slices_of(features):
        cols = pl.ds(start, size)
        normed = (hidden[:, cols] * scale * gain[:, cols]).astype(jnp.bfloat16)
        packed[:, cols] = normed
        logits = logits + lax.dot_general(normed, router[:, cols], last_dims, preferred_element_type=jnp.float32)
    label = lax.broadcasted_iota(jnp.int32, (experts, rows), 0)
    marks = sum((ids[k : k + 1, :] == label).astype(jnp.float32) for k in range(TOP))
    eye = (
        lax.broadcasted_iota(jnp.int32, (rows, rows), 0) == lax.broadcasted_iota(jnp.int32, (rows, rows), 1)
    ).astype(jnp.float32)
    named = lax.dot_general(eye, marks, last_dims, preferred_element_type=jnp.float32) > 0.5
    peak = jnp.max(jnp.where(named, logits, -jnp.inf), axis=1, keepdims=True)
    grown = jnp.where(named, jnp.exp(jnp.where(named, logits - peak, 0.0)), 0.0)
    probs = grown / jnp.sum(grown, axis=1, keepdims=True)
    packed[:, features:] = jnp.zeros((rows, packed.shape[1] - features), jnp.bfloat16)
    packed[:, features : features + experts] = probs.astype(jnp.bfloat16)
    for j in range(1, count):
        exchange(j, True).wait_send()


def project(side, queries, new_keys, new_values, cache_keys, cache_values, cache_len, out_proj, resid, gain, router, ids):
    rows, width = resid.shape
    count = 2 * side * side
    dma, bf = pltpu.SemaphoreType.DMA, jnp.bfloat16
    vmem, anywhere = pl.BlockSpec(memory_space=pltpu.VMEM), pl.BlockSpec(memory_space=pl.ANY)
    return pl.pallas_call(
        lambda *refs: projection_kernel(side, *refs),
        out_shape=(
            jax.ShapeDtypeStruct((rows, width), jnp.float32),
            jax.ShapeDtypeStruct((rows, width + pl.cdiv(router.shape[0], 128) * 128), bf),
        ),
        in_specs=[vmem, vmem, vmem, anywhere, anywhere, pl.BlockSpec(memory_space=pltpu.SMEM), anywhere]
        + [vmem] * 4,
        out_specs=(vmem, vmem),
        scratch_shapes=[
            pltpu.VMEM((count, H // count, rows, HD), bf),
            pltpu.VMEM(cache_keys.shape, bf),
            pltpu.VMEM(cache_values.shape, bf),
            pltpu.VMEM((H * rows, HD), jnp.float32),
            pltpu.VMEM((H * rows, HD), jnp.float32),
            pltpu.VMEM(new_keys.shape, jnp.float32),
            pltpu.VMEM(new_values.shape, jnp.float32),
            pltpu.VMEM(out_proj.shape, bf),
            pltpu.VMEM((count, H // count, rows, HD), bf),
            pltpu.VMEM((side, side, 2, rows, width), bf),
            dma((3,)),
            dma((count,)),
            dma((count,)),
        ]
        + reduce_shapes(side, 1, rows, width),
        compiler_params=pltpu.CompilerParams(
            collective_id=0, has_side_effects=True, vmem_limit_bytes=VMEM_LIMIT
        ),
    )(queries, new_keys, new_values, cache_keys, cache_values, cache_len, out_proj, resid, gain, router, ids)


AXES = ("y", "x", "z")
TURNS = (("x", "y", "z"), ("y", "z", "x"), ("z", "x", "y"))
ORDERS = TURNS * 3
WIDTHS = (512,) * 6 + (384, 384, 256)
STARTS = tuple(sum(WIDTHS[:s]) for s in range(len(WIDTHS)))


class Spot:
    def __init__(self):
        ep = lax.axis_index("ep")
        self.core = lax.rem(ep, 2)
        self.pos = {"x": lax.rem(ep // 2, 4), "y": ep // 8, "z": lax.axis_index("dp")}

    def coord(self, axis, off):
        return lax.rem(self.pos[axis] + off, 4) if off else self.pos[axis]

    def at(self, axis=None, off=0, flip=False):
        place = dict(self.pos)
        if axis:
            place[axis] = self.coord(axis, off)
        core = 1 - self.core if flip else self.core
        return ((place["y"] * 4 + place["x"]) * 2 + core, place["z"])

    def index(self, fixed):
        return tuple(fixed.get(axis, slice(None)) for axis in AXES)


def expert_kernel(own, gate_hbm, up_hbm, down_hbm, mixed, *scratch):
    n = len(ORDERS)
    gu, down, act, total, wsem, nsem, fsem, csem, rnear, rfar, rcore = scratch[:11]
    scratch = scratch[11:]
    held, inner = scratch[:n], scratch[n : 2 * n]
    nears = [scratch[2 * n + 3 * s : 2 * n + 3 * s + 3] for s in range(n)]
    fars = [scratch[5 * n + 3 * s : 5 * n + 3 * s + 3] for s in range(n)]
    here = Spot()
    rows = own.shape[0]
    hidden = act.shape[1]
    loads = [
        pltpu.make_async_copy(gate_hbm.at[0], gu.at[:, pl.ds(0, hidden)], wsem.at[0]),
        pltpu.make_async_copy(up_hbm.at[0], gu.at[:, pl.ds(hidden, hidden)], wsem.at[1]),
        pltpu.make_async_copy(down_hbm.at[0], down, wsem.at[2]),
    ]
    for load in loads:
        load.start()
    greet([here.at(flip=True)] + [here.at(axis, off) for axis in AXES for off in (1, 2, 3)])
    sends = []

    def go(copy):
        copy.start()
        sends.append(copy)

    def cols_of(s):
        return pl.ds(STARTS[s], held[s].shape[-1])

    def halves(width, d):
        cut = 256 if width > 256 else 128
        return (slice(None), pl.ds(0, cut) if d == 0 else pl.ds(cut, width - cut))

    def spread_index(s, p, off, core=None):
        order = ORDERS[s]
        fixed = {axis: here.pos[axis] for axis in order[p + 1 :]}
        fixed[order[p]] = here.coord(order[p], off)
        return (here.core if core is None else core,) + here.index(fixed)

    def spread(s, p, off, core=None):
        return held[s].at[spread_index(s, p, off, core)]

    def spread_half(s, p, off, d):
        width = held[s].shape[-1]
        return held[s].at[spread_index(s, p, off) + halves(width, d)]

    def direct_gather(s, p):
        return p == 0 or (p == 1 and s < 3) or (p == 2 and s >= 6)

    def near_gather(s, p, d, h, sending):
        axis = ORDERS[s][p]
        off = (1, 3)[d]
        ref = spread_half(s, p, 0 if sending else 4 - off, h)
        return remote(
            ref, ref, nsem.at[s, p, d, h, 0], nsem.at[s, p, d, h, 1], here.at(axis, off if sending else 4 - off)
        )

    def gather_near(s, p):
        axis = ORDERS[s][p]
        for h in range(2):
            for d in range(2):
                go(near_gather(s, p, d, (d + h) % 2, True))
        if direct_gather(s, p):
            ref = spread(s, p, 0)
            go(remote(ref, ref, fsem.at[s, p, 0, 0], fsem.at[s, p, 0, 1], here.at(axis, 2)))
        if p == 2:
            give(s, 0, 0)

    def gather_far(s, p):
        axis = ORDERS[s][p]
        for d, (off, back) in enumerate(((1, 3), (3, 1))):
            near_gather(s, p, d, d, False).wait_recv()
            if not direct_gather(s, p):
                ref = spread_half(s, p, back, d)
                go(remote(ref, ref, fsem.at[s, p, d, 0], fsem.at[s, p, d, 1], here.at(axis, off)))

    def gather_end(s, p):
        axis = ORDERS[s][p]
        for d, back in enumerate((3, 1)):
            near_gather(s, p, d, 1 - d, False).wait_recv()
            if p == 2:
                give(s, 1 + d, back)
        if direct_gather(s, p):
            ref = spread(s, p, 2)
            remote(ref, ref, fsem.at[s, p, 0, 0], fsem.at[s, p, 0, 1], here.at(axis, 2)).wait_recv()
        else:
            for d, back in enumerate((3, 1)):
                ref = spread_half(s, p, 2, d)
                remote(ref, ref, fsem.at[s, p, d, 0], fsem.at[s, p, d, 1], here.at(axis, back)).wait_recv()
        if p == 2:
            give(s, 3, 2)

    def give(s, k, off):
        ref = spread(s, 2, off)
        go(remote(ref, ref, csem.at[s, k, 0], csem.at[s, k, 1], here.at(flip=True)))

    def take(s):
        for k, off in enumerate((0, 3, 1, 2)):
            ref = spread(s, 2, off, 1 - here.core)
            remote(ref, ref, csem.at[s, k, 0], csem.at[s, k, 1], here.at(flip=True)).wait_recv()

    group = 32 * rows

    def rows_at(i):
        return pl.ds(pl.multiple_of(i * group, group), group)

    def span(s):
        return slice(STARTS[s], STARTS[s] + WIDTHS[s])

    def consume(s):
        if s == 0:
            loads[0].wait()
            loads[1].wait()

        def step(i, carry):
            block = held[s][i // 2, pl.ds(2 * lax.rem(i, 2), 2), :, :, :, : WIDTHS[s]].reshape(group, WIDTHS[s])
            value = jnp.dot(block, gu[span(s), :], preferred_element_type=jnp.float32)
            total[rows_at(i), :] = value if s == 0 else total[rows_at(i), :] + value
            return carry

        lax.fori_loop(0, 4, step, 0)

    def start(s):
        held[s][here.core, here.pos["y"], here.pos["x"], here.pos["z"]] = own[:, cols_of(s)]
        gather_near(s, 0)

    def second(s):
        gather_far(s, 0)
        gather_end(s, 0)
        gather_near(s, 1)

    def second_far(s):
        gather_far(s, 1)

    def third(s):
        gather_end(s, 1)
        gather_near(s, 2)

    def third_far(s):
        gather_far(s, 2)

    def last(s):
        gather_end(s, 2)

    def use(s):
        take(s)
        consume(s)

    def run(*steps):
        for phase, group_of in steps:
            for s in group_of:
                phase(s)

    run(
        (start, range(n)), (second, (0, 1, 2)), (second, (3, 4, 5)), (second_far, (0, 1, 2)), (third, (0, 1, 2)),
        (second_far, (3, 4, 5)), (second, (6, 7, 8)), (third_far, (0, 1, 2)), (third, (3, 4, 5)),
        (second_far, (6, 7, 8)), (last, (0, 1, 2)),
    )
    for s in range(3):
        run((use, (s,)), (third_far, (3 + s,)), (third, (6 + s,)))
    run((last, (3, 4, 5)))
    for s in range(3, 6):
        run((use, (s,)), (third_far, (3 + s,)))
    run((last, (6, 7, 8)), (use, (6, 7, 8)))
    for copy in sends:
        copy.wait_send()
    sends.clear()
    loads[2].wait()
    expert = (lax.axis_index("ep") * 4 + here.pos["z"]) // 2

    def activate(i, carry):
        tail = held[n - 1][i // 2, pl.ds(2 * lax.rem(i, 2), 2), :, :, :, WIDTHS[n - 1] :].reshape(group, 128)
        lane = lax.broadcasted_iota(jnp.int32, tail.shape, 1)
        weight = jnp.sum(jnp.where(lane == expert, tail.astype(jnp.float32), 0.0), axis=1, keepdims=True)
        gate_val = total[rows_at(i), :hidden]
        value = gate_val / (1.0 + jnp.exp(-gate_val)) * total[rows_at(i), hidden:] * weight
        act[rows_at(i), :] = value.astype(jnp.bfloat16)
        return carry

    lax.fori_loop(0, 4, activate, 0)

    def fold(s, p, off):
        order = ORDERS[s][::-1]
        fixed = {axis: here.pos[axis] for axis in order[:p]}
        fixed[order[p]] = here.coord(order[p], off)
        return here.index(fixed)

    def direct_fold(s, p):
        return p >= 1

    def gain(s, p, off):
        index = fold(s, p, off)
        if p == 0:
            mine = held[s][(here.core,) + index + (slice(None), pl.ds(0, WIDTHS[s]))]
            return mine + inner[s][index]
        return inner[s][index]

    def core_copy(s):
        return remote(
            held[s].at[1 - here.core, :, :, :, :, pl.ds(0, WIDTHS[s])],
            inner[s],
            rcore.at[s, 0],
            rcore.at[s, 1],
            here.at(flip=True),
        )

    def produce(s):
        def step(core):
            def one(h, carry):
                i = 2 * core + h
                value = jnp.dot(
                    act[rows_at(i), :], down[:, span(s)], preferred_element_type=jnp.float32
                )
                held[s][core, pl.ds(2 * h, 2), :, :, :, : WIDTHS[s]] = value.astype(jnp.bfloat16).reshape(
                    2, 4, 4, rows, WIDTHS[s]
                )
                return carry

            lax.fori_loop(0, 2, one, 0)

        step(1 - here.core)
        go(core_copy(s))
        step(here.core)

    def half_of(s, ref, index, d):
        return ref.at[index + halves(WIDTHS[s], d)]

    def lead(p):
        return (slice(None),) * (2 - p)

    def far_copy(s, p, d, sending):
        axis = ORDERS[s][2 - p]
        index = fold(s, p, 2)
        if direct_fold(s, p):
            return remote(
                inner[s].at[index], fars[s][p], rfar.at[s, p, 0, 0], rfar.at[s, p, 0, 1], here.at(axis, 2)
            )
        return remote(
            half_of(s, inner[s], index, d),
            half_of(s, fars[s][p], lead(p), d),
            rfar.at[s, p, d, 0],
            rfar.at[s, p, d, 1],
            here.at(axis, (1, 3)[d]),
        )

    def near_copy(s, p, d, h):
        axis = ORDERS[s][2 - p]
        off = (1, 3)[d]
        return remote(
            half_of(s, inner[s], fold(s, p, off), h),
            half_of(s, nears[s][p], (d,) + lead(p), h),
            rnear.at[s, p, d, h, 0],
            rnear.at[s, p, d, h, 1],
            here.at(axis, off),
        )

    def fold_far(s, p):
        if p == 0:
            core_copy(s).wait_recv()
            inner[s][fold(s, 0, 2)] = gain(s, 0, 2)
        for d in range(1 if direct_fold(s, p) else 2):
            go(far_copy(s, p, d, True))
        for d, off in enumerate((1, 3)):
            if p == 0:
                inner[s][fold(s, p, off)] = gain(s, p, off)
            go(near_copy(s, p, d, 1 - d))
            if direct_fold(s, p):
                go(near_copy(s, p, d, d))

    def fold_near(s, p):
        for d, off in enumerate((1, 3)):
            far_copy(s, p, d, False).wait_recv()
            part = fold(s, p, off) + halves(WIDTHS[s], d)
            inner[s][part] = inner[s][part] + fars[s][p][lead(p) + halves(WIDTHS[s], d)]
            go(near_copy(s, p, d, d))

    def fold_end(s, p):
        value = gain(s, p, 0).astype(jnp.float32)
        for d in range(2):
            for h in range(2):
                near_copy(s, p, d, h).wait_recv()
            value = value + nears[s][p][d].astype(jnp.float32)
        if direct_fold(s, p):
            far_copy(s, p, 0, False).wait_recv()
            value = value + fars[s][p][...].astype(jnp.float32)
        if p == 2:
            mixed[:, span(s)] = value
        else:
            inner[s][fold(s, p, 0)] = value.astype(jnp.bfloat16)

    def next_fold(s, p):
        fold_end(s, p - 1)
        fold_far(s, p)

    phases = (
        (produce, 0),
        (lambda s: fold_far(s, 0), 1),
        (lambda s: fold_near(s, 0), 3),
        (lambda s: next_fold(s, 1), 5),
        (lambda s: next_fold(s, 2), 7),
        (lambda s: fold_end(s, 2), 9),
    )
    for step in range(n + phases[-1][1]):
        for phase, lag in phases:
            if 0 <= step - lag < n:
                phase(step - lag)
    for copy in sends:
        copy.wait_send()


def run_experts(packed, gate_slab, up_slab, down_slab):
    rows, width = packed.shape[0], down_slab.shape[2]
    hidden = gate_slab.shape[2]
    n = len(ORDERS)
    dma, bf = pltpu.SemaphoreType.DMA, jnp.bfloat16
    vmem, anywhere = pl.BlockSpec(memory_space=pltpu.VMEM), pl.BlockSpec(memory_space=pl.ANY)
    extra = packed.shape[1] - width
    shapes = [
        pltpu.VMEM((gate_slab.shape[1], 2 * hidden), bf),
        pltpu.VMEM(down_slab.shape[1:], bf),
        pltpu.VMEM((128 * rows, hidden), bf),
        pltpu.VMEM((128 * rows, 2 * hidden), jnp.float32),
        dma((3,)),
        dma((n, 3, 2, 2, 2)),
        dma((n, 3, 2, 2)),
        dma((n, 4, 2)),
        dma((n, 3, 2, 2, 2)),
        dma((n, 3, 2, 2)),
        dma((n, 2)),
    ]
    shapes += [pltpu.VMEM((2, 4, 4, 4, rows, w + extra * (s == n - 1)), bf) for s, w in enumerate(WIDTHS)]
    shapes += [pltpu.VMEM((4, 4, 4, rows, w), bf) for w in WIDTHS]
    shapes += [pltpu.VMEM((2,) + (4,) * (2 - p) + (rows, w), bf) for w in WIDTHS for p in range(3)]
    shapes += [pltpu.VMEM((4,) * (2 - p) + (rows, w), bf) for w in WIDTHS for p in range(3)]
    return pl.pallas_call(
        expert_kernel,
        out_shape=jax.ShapeDtypeStruct((rows, width), jnp.float32),
        in_specs=[vmem, anywhere, anywhere, anywhere],
        out_specs=vmem,
        scratch_shapes=shapes,
        compiler_params=pltpu.CompilerParams(
            collective_id=1, has_side_effects=True, vmem_limit_bytes=VMEM_LIMIT
        ),
    )(packed, gate_slab, up_slab, down_slab)


def local(
    resid,
    queries,
    new_keys,
    new_values,
    cache_keys,
    cache_values,
    cache_len,
    out_proj,
    norm_gain,
    router,
    expert_ids,
    gate_slab,
    up_slab,
    down_slab,
):
    side = math.isqrt(lax.axis_size("ep") // 2)
    hidden, packed = project(
        side, queries, new_keys, new_values, cache_keys, cache_values, cache_len,
        out_proj, resid, norm_gain.reshape(1, -1), router.T, expert_ids.T,
    )
    return hidden + run_experts(packed, gate_slab, up_slab, down_slab)


def solution(mesh):
    in_specs = (
        P(("ep", "dp"), None),
        P(("ep", "dp"), None),
        P(("ep", "dp"), None),
        P(("ep", "dp"), None),
        P(("ep", "dp"), None, None),
        P(("ep", "dp"), None, None),
        P(("ep", "dp")),
        P("ep", None),
        P(),
        P(),
        P(("ep", "dp"), None),
        P(("ep", "dp"), None, None),
        P(("ep", "dp"), None, None),
        P(("ep", "dp"), None, None),
    )
    out_specs = P(("ep", "dp"), None)
    return jax.shard_map(local, mesh=mesh, in_specs=in_specs, out_specs=out_specs, check_vma=False)
```

```python
import math

import jax
import jax.numpy as jnp
from jax import lax
from jax.experimental import pallas as pl
from jax.experimental.pallas import tpu as pltpu
from jax.sharding import PartitionSpec as P

D = 4096
H = 64
KVH = 4
HD = 128
TOP = 8
CAP = 4


MESH = pl.DeviceIdType.MESH
VMEM_LIMIT = 66_000_000


def remote(src, dst, send, recv, device):
    return pltpu.make_async_remote_copy(
        src_ref=src, dst_ref=dst, send_sem=send, recv_sem=recv, device_id=device, device_id_type=MESH
    )


def attend(queries, new_keys, new_values, keys, values, lengths, attended, qs, os, nk, nv):
    tokens = queries.shape[0]
    share = H // KVH
    scale = 1.0 / math.sqrt(HD)
    for h in range(H):
        qs[tokens * h : tokens * h + tokens, :] = queries[:, HD * h : HD * h + HD].astype(jnp.float32)
    nk[...] = new_keys[...].astype(jnp.float32)
    nv[...] = new_values[...].astype(jnp.float32)

    def spread(row):
        return jnp.concatenate(
            [jnp.broadcast_to(row[:, HD * g : HD * g + HD], (share, HD)) for g in range(KVH)], axis=0
        )

    def one(t):
        rows = pl.ds(t, H, stride=tokens)
        query = qs[rows, :]
        narrow = query.astype(jnp.bfloat16)
        scores = jnp.concatenate(
            [
                lax.dot_general(
                    narrow[share * g : share * g + share],
                    keys[t, :, HD * g : HD * g + HD],
                    (((1,), (1,)), ((), ())),
                    preferred_element_type=jnp.float32,
                )
                for g in range(KVH)
            ],
            axis=0,
        )
        own = jnp.sum(query * spread(nk[pl.ds(t, 1), :]), axis=1, keepdims=True) * scale
        valid = lax.broadcasted_iota(jnp.int32, scores.shape, 1) < lengths[t]
        scores = jnp.where(valid, scores * scale, -1e30)
        peak = jnp.maximum(jnp.max(scores, axis=1, keepdims=True), own)
        grown = jnp.exp(scores - peak)
        own_grown = jnp.exp(own - peak)
        denom = jnp.sum(grown, axis=1, keepdims=True) + own_grown
        weights = (grown / denom).astype(jnp.bfloat16)
        own_weight = (own_grown / denom).astype(jnp.bfloat16).astype(jnp.float32)
        blended = jnp.concatenate(
            [
                jnp.dot(
                    weights[share * g : share * g + share],
                    values[t, :, HD * g : HD * g + HD],
                    preferred_element_type=jnp.float32,
                )
                for g in range(KVH)
            ],
            axis=0,
        )
        os[rows, :] = blended + own_weight * spread(nv[pl.ds(t, 1), :])

    def several(i, carry):
        for k in range(4):
            one(4 * i + k)
        return carry

    lax.fori_loop(0, tokens // 4, several, 0)
    attended[...] = os[...].astype(jnp.bfloat16).reshape(attended.shape)


AXES = ("y", "x", "z")
TURNS = (("x", "y", "z"), ("y", "z", "x"), ("z", "x", "y"))
ORDERS = TURNS * 3
WIDTHS = (512,) * 6 + (384, 384, 256)
STARTS = tuple(sum(WIDTHS[:s]) for s in range(len(WIDTHS)))


class Spot:
    def __init__(self):
        ep = lax.axis_index("ep")
        self.core = lax.rem(ep, 2)
        self.pos = {"x": lax.rem(ep // 2, 4), "y": ep // 8, "z": lax.axis_index("dp")}

    def coord(self, axis, off):
        return lax.rem(self.pos[axis] + off, 4) if off else self.pos[axis]

    def at(self, axis=None, off=0, flip=False):
        place = dict(self.pos)
        if axis:
            place[axis] = self.coord(axis, off)
        core = 1 - self.core if flip else self.core
        return ((place["y"] * 4 + place["x"]) * 2 + core, place["z"])

    def plane(self, dy, dx):
        return ((self.coord("y", dy) * 4 + self.coord("x", dx)) * 2 + self.core, self.pos["z"])

    def index(self, fixed):
        return tuple(fixed.get(axis, slice(None)) for axis in AXES)


LAGS = (0, 2, 5, 8)


def layer_kernel(
    queries, new_keys, new_values, keys_hbm, values_hbm, lengths, weight_hbm, resid, gain, router, ids,
    gate_hbm, up_hbm, down_hbm, mixed,
    own, attended, keys, values, qs, os, nk, nv, weight, regrouped, in2, sum2, in3, asem, osem, psem, qsem, tsem,
    gu, down, act, total, picked, sel, back, wsem, nsem, fsem, csem, rnear, rfar, rcore, *scratch
):
    n = len(ORDERS)
    held, inner = scratch[:n], scratch[n : 2 * n]
    nears = [scratch[2 * n + 3 * s : 2 * n + 3 * s + 3] for s in range(n)]
    fars = [scratch[5 * n + 3 * s : 5 * n + 3 * s + 3] for s in range(n)]
    here = Spot()
    rows = own.shape[0]
    hidden = act.shape[1]
    experts = router.shape[0]
    count = 32
    ep, z = lax.axis_index("ep"), lax.axis_index("dp")
    caches = [
        pltpu.make_async_copy(keys_hbm, keys, asem.at[0]),
        pltpu.make_async_copy(values_hbm, values, asem.at[1]),
        pltpu.make_async_copy(weight_hbm, weight, asem.at[2]),
    ]
    loads = [
        pltpu.make_async_copy(gate_hbm.at[0], gu.at[:, pl.ds(0, hidden)], wsem.at[0]),
        pltpu.make_async_copy(up_hbm.at[0], gu.at[:, pl.ds(hidden, hidden)], wsem.at[1]),
        pltpu.make_async_copy(down_hbm.at[0], down, wsem.at[2]),
    ]
    for load in caches + loads:
        load.start()

    def peer(j):
        return lax.rem(ep + j, count)

    barrier = pltpu.get_barrier_semaphore()
    everyone = [(peer(j), z) for j in range(1, count)] + [here.at("z", off) for off in (1, 2, 3)]
    for device in everyone:
        pl.semaphore_signal(barrier, inc=1, device_id=device, device_id_type=MESH)
    caches[0].wait()
    caches[1].wait()
    attend(queries, new_keys, new_values, keys, values, lengths, attended, qs, os, nk, nv)
    pl.semaphore_wait(barrier, len(everyone))
    sends, early = [], []

    def go(copy, kept=sends):
        copy.start()
        kept.append(copy)

    for j in range(1, count):
        go(remote(attended.at[peer(j)], regrouped.at[ep], osem.at[j, 0], osem.at[count - j, 1], (peer(j), z)), early)
    regrouped[ep] = attended[ep]
    caches[2].wait()
    for j in range(1, count):
        remote(attended.at[peer(j)], regrouped.at[peer(j)], osem.at[j, 0], osem.at[j, 1], (peer(j), z)).wait_recv()

    def pair_copy(s):
        return remote(
            inner[s].at[:, :, 1 - here.core], inner[s].at[:, :, 2], psem.at[s, 0], psem.at[s, 1], here.at(flip=True)
        )

    def turn(s, a, b):
        return (a, b) if s % 2 == 0 else (b, a)

    def line(s, a, b):
        dy, dx = turn(s, a, b)
        return here.coord("y", dy), here.coord("x", dx)

    def columns(s):
        return pl.ds(STARTS[s], WIDTHS[s])

    def first_copy(s, ja, kb, sending):
        y, x = line(s, ja, kb)
        return remote(
            inner[s].at[y, x, 2],
            in2.at[3 - ja, kb, :, columns(s)],
            qsem.at[s, ja, kb, 0],
            qsem.at[s, 4 - ja if sending else ja, kb, 1],
            here.plane(*turn(s, ja, 0)),
        )

    def second_copy(s, kb, sending):
        return remote(
            sum2.at[kb, :, columns(s)],
            in3.at[3 - kb, :, columns(s)],
            tsem.at[s, kb, 0],
            tsem.at[s, 4 - kb if sending else kb, 1],
            here.plane(*turn(s, 0, kb)),
        )

    def wide(value):
        return value.astype(jnp.float32)

    def phase0(s):
        left = jnp.concatenate([regrouped[:, k].reshape(count * rows, HD) for k in range(2)], axis=1)
        value = jnp.dot(left, weight[:, columns(s)], preferred_element_type=jnp.float32)
        inner[s][:, :, 0:2] = value.astype(jnp.bfloat16).reshape(4, 4, 2, rows, WIDTHS[s])
        go(pair_copy(s), early)

    def phase1(s):
        pair_copy(s).wait_recv()
        for a in (1, 2, 3, 0):
            for b in (1, 2, 3, 0):
                y, x = line(s, a, b)
                inner[s][y, x, 2] = (wide(inner[s][y, x, here.core]) + wide(inner[s][y, x, 2])).astype(jnp.bfloat16)
                if a:
                    go(first_copy(s, a, b, True), early)

    def phase2(s):
        for b in (1, 2, 3, 0):
            y, x = line(s, 0, b)
            value = wide(inner[s][y, x, 2])
            for a in range(1, 4):
                first_copy(s, a, b, False).wait_recv()
                value = value + wide(in2[a - 1, b, :, columns(s)])
            sum2[b, :, columns(s)] = value.astype(jnp.bfloat16)
            if b:
                go(second_copy(s, b, True), early)

    def phase3(s):
        value = wide(sum2[0, :, columns(s)])
        for b in range(1, 4):
            second_copy(s, b, False).wait_recv()
            value = value + wide(in3[b - 1, :, columns(s)])
        value = wide(resid[:, columns(s)]) + value
        mixed[:, columns(s)] = value
        squares.append(jnp.sum(value * value, axis=1, keepdims=True))
        scaled = (value * gain[:, columns(s)]).astype(jnp.bfloat16)
        own[:, columns(s)] = scaled
        logits.append(
            lax.dot_general(scaled, router[:, columns(s)], (((1,), (1,)), ((), ())), preferred_element_type=jnp.float32)
        )
        if s < n - 1:
            start(s)
        if s >= 3:
            second(s - 3)
        if s >= 6:
            second_far(s - 6)
            third(s - 6)

    def find():
        label = lax.broadcasted_iota(jnp.int32, (experts, rows), 0)
        marks = sum((ids[k : k + 1, :] == label).astype(jnp.float32) for k in range(TOP))
        eye = (
            lax.broadcasted_iota(jnp.int32, (rows, rows), 0) == lax.broadcasted_iota(jnp.int32, (rows, rows), 1)
        ).astype(jnp.float32)
        return lax.dot_general(eye, marks, (((1,), (1,)), ((), ())), preferred_element_type=jnp.float32) > 0.5

    def route(named, logit):
        peak = jnp.max(jnp.where(named, logit, -jnp.inf), axis=1, keepdims=True)
        grown = jnp.where(named, jnp.exp(jnp.where(named, logit - peak, 0.0)), 0.0)
        return grown / jnp.sum(grown, axis=1, keepdims=True)

    def halves(width, d):
        cut = 256 if width > 256 else 128
        return (slice(None), pl.ds(0, cut) if d == 0 else pl.ds(cut, width - cut))

    def spread_index(s, p, off, core=None):
        order = ORDERS[s]
        fixed = {axis: here.pos[axis] for axis in order[p + 1 :]}
        fixed[order[p]] = here.coord(order[p], off)
        return (here.core if core is None else core,) + here.index(fixed)

    def spread(s, p, off, core=None):
        return held[s].at[spread_index(s, p, off, core)]

    def spread_half(s, p, off, d):
        width = held[s].shape[-1]
        return held[s].at[spread_index(s, p, off) + halves(width, d)]

    def direct_gather(s, p):
        return p == 0 or (p == 1 and s < 3) or (p == 2 and s >= 6)

    def near_gather(s, p, d, h, sending):
        axis = ORDERS[s][p]
        off = (1, 3)[d]
        ref = spread_half(s, p, 0 if sending else 4 - off, h)
        return remote(
            ref, ref, nsem.at[s, p, d, h, 0], nsem.at[s, p, d, h, 1], here.at(axis, off if sending else 4 - off)
        )

    def gather_near(s, p):
        axis = ORDERS[s][p]
        for h in range(2):
            for d in range(2):
                go(near_gather(s, p, d, (d + h) % 2, True))
        if direct_gather(s, p):
            ref = spread(s, p, 0)
            go(remote(ref, ref, fsem.at[s, p, 0, 0], fsem.at[s, p, 0, 1], here.at(axis, 2)))
        if p == 2:
            give(s, 0, 0)

    def gather_far(s, p):
        axis = ORDERS[s][p]
        for d, (off, back) in enumerate(((1, 3), (3, 1))):
            near_gather(s, p, d, d, False).wait_recv()
            if not direct_gather(s, p):
                ref = spread_half(s, p, back, d)
                go(remote(ref, ref, fsem.at[s, p, d, 0], fsem.at[s, p, d, 1], here.at(axis, off)))

    def gather_end(s, p):
        axis = ORDERS[s][p]
        for d, back in enumerate((3, 1)):
            near_gather(s, p, d, 1 - d, False).wait_recv()
            if p == 2:
                give(s, 1 + d, back)
        if direct_gather(s, p):
            ref = spread(s, p, 2)
            remote(ref, ref, fsem.at[s, p, 0, 0], fsem.at[s, p, 0, 1], here.at(axis, 2)).wait_recv()
        else:
            for d, back in enumerate((3, 1)):
                ref = spread_half(s, p, 2, d)
                remote(ref, ref, fsem.at[s, p, d, 0], fsem.at[s, p, d, 1], here.at(axis, back)).wait_recv()
        if p == 2:
            give(s, 3, 2)

    def give(s, k, off):
        ref = spread(s, 2, off)
        go(remote(ref, ref, csem.at[s, k, 0], csem.at[s, k, 1], here.at(flip=True)))

    def take(s):
        for k, off in enumerate((0, 3, 1, 2)):
            ref = spread(s, 2, off, 1 - here.core)
            remote(ref, ref, csem.at[s, k, 0], csem.at[s, k, 1], here.at(flip=True)).wait_recv()

    group = 32 * rows
    block = 16 * rows
    slots = 16 * CAP
    mine = (ep * 4 + z) // 2

    def rows_at(i):
        return pl.ds(pl.multiple_of(i * group, group), group)

    def span(s):
        return slice(STARTS[s], STARTS[s] + WIDTHS[s])

    def lane_of(value, wanted):
        lane = lax.broadcasted_iota(jnp.int32, value.shape, 1)
        return jnp.sum(jnp.where(wanted(lane), value, 0.0), axis=1, keepdims=True)

    def select():
        row = lax.broadcasted_iota(jnp.int32, (block, block), 0)
        col = lax.broadcasted_iota(jnp.int32, (block, block), 1)
        earlier = ((row // rows == col // rows) & (col < row)).astype(jnp.bfloat16)
        token = lax.broadcasted_iota(jnp.int32, (block, slots), 0)
        slot = lax.broadcasted_iota(jnp.int32, (block, slots), 1)
        near = token // rows == slot // CAP
        turn_of = lax.rem(slot, CAP).astype(jnp.float32)
        eye = (
            lax.broadcasted_iota(jnp.int32, (slots, slots), 0) == lax.broadcasted_iota(jnp.int32, (slots, slots), 1)
        ).astype(jnp.bfloat16)

        def one(i, carry):
            marks = held[0][i // 4, lax.rem(i, 4), :, :, :, WIDTHS[0] :].reshape(block, 128)
            rank = lane_of(
                jnp.dot(earlier, marks, preferred_element_type=jnp.float32), lambda lane: lane == mine
            )
            chosen = lane_of(marks.astype(jnp.float32), lambda lane: lane == mine)
            hit = jnp.where(near & (rank == turn_of), chosen, 0.0).astype(jnp.bfloat16)
            back[i] = hit
            sel[i] = lax.dot_general(
                eye, hit, (((1,), (1,)), ((), ())), preferred_element_type=jnp.float32
            ).astype(jnp.bfloat16)
            return carry

        lax.fori_loop(0, 8, one, 0)

    def tokens_of(s, i, cols):
        return held[s][i // 4, i % 4, :, :, :, cols].reshape(block, cols.stop - cols.start)

    def consume(s):
        if s == 0:
            select()
            loads[0].wait()
            loads[1].wait()
        width = WIDTHS[s]
        for i in range(8):
            chosen = jnp.dot(sel[i], tokens_of(s, i, slice(0, width)), preferred_element_type=jnp.float32)
            picked[slots * i : slots * i + slots, :width] = chosen.astype(jnp.bfloat16)
        for i in range(2):
            part = slice(4 * slots * i, 4 * slots * (i + 1))
            value = jnp.dot(picked[part, :width], gu[span(s), :], preferred_element_type=jnp.float32)
            total[part, :] = value if s == 0 else total[part, :] + value

    def start(s):
        place = (here.core, here.pos["y"], here.pos["x"], here.pos["z"], slice(None))
        held[s][place + (pl.ds(0, WIDTHS[s]),)] = own[:, columns(s)]
        if s == 0:
            held[s][place + (pl.ds(WIDTHS[s], 128),)] = own[:, pl.ds(D, 128)]
        if s == n - 1:
            held[s][place + (pl.ds(WIDTHS[s], 128),)] = own[:, pl.ds(D + 128, 128)]
        gather_near(s, 0)

    def second(s):
        gather_far(s, 0)
        gather_end(s, 0)
        gather_near(s, 1)

    def second_far(s):
        gather_far(s, 1)

    def third(s):
        gather_end(s, 1)
        gather_near(s, 2)

    def third_far(s):
        gather_far(s, 2)

    def last(s):
        gather_end(s, 2)

    def use(s):
        take(s)
        consume(s)

    def run(*steps):
        for phase, group_of in steps:
            for s in group_of:
                phase(s)

    squares, logits = [], []
    named = find()
    own[:, D : D + 128] = jnp.concatenate(
        [named.astype(jnp.float32), jnp.zeros((rows, 128 - experts), jnp.float32)], axis=1
    ).astype(jnp.bfloat16)
    for step in range(n + LAGS[-1]):
        for phase, lag in zip((phase0, phase1, phase2, phase3), LAGS):
            if 0 <= step - lag < n:
                phase(step - lag)
    for copy in early:
        copy.wait_send()
    scale = lax.rsqrt(jnp.maximum(sum(squares) / D, 0.25))
    probs = route(named, sum(logits) * scale)
    high = scale.astype(jnp.bfloat16)
    low = scale - high.astype(jnp.float32)
    lane = lax.broadcasted_iota(jnp.int32, (rows, 128 - experts), 1)
    tail = jnp.where(lane == 0, high.astype(jnp.float32), jnp.where(lane == 1, low, 0.0))
    own[:, D + 128 :] = jnp.concatenate([probs, tail], axis=1).astype(jnp.bfloat16)
    run(
        (start, (8,)), (second_far, (3, 4, 5)), (second, (6, 7, 8)), (third_far, (0, 1, 2)), (third, (3, 4, 5)),
        (second_far, (6, 7, 8)), (last, (0, 1, 2)),
    )
    for s in range(3):
        run((use, (s,)), (third_far, (3 + s,)), (third, (6 + s,)))
    run((last, (3, 4, 5)))
    for s in range(3, 6):
        run((use, (s,)), (third_far, (3 + s,)))
    run((last, (6, 7, 8)), (use, (6, 7, 8)))
    for copy in sends:
        copy.wait_send()
    sends.clear()
    loads[2].wait()
    for i in range(8):
        tail = tokens_of(n - 1, i, slice(WIDTHS[n - 1], WIDTHS[n - 1] + 128))
        tail = jnp.dot(sel[i], tail, preferred_element_type=jnp.float32)
        prob = lane_of(tail, lambda lane: lane == mine)
        factor = lane_of(tail, lambda lane: lane // 2 == experts // 2)
        part = slice(slots * i, slots * i + slots)
        gate_val = total[part, :hidden] * factor
        value = gate_val / (1.0 + jnp.exp(-gate_val)) * (total[part, hidden:] * factor) * prob
        act[block * i : block * i + block, :] = jnp.dot(
            back[i], value.astype(jnp.bfloat16), preferred_element_type=jnp.float32
        ).astype(jnp.bfloat16)

    def fold(s, p, off):
        order = ORDERS[s][::-1]
        fixed = {axis: here.pos[axis] for axis in order[:p]}
        fixed[order[p]] = here.coord(order[p], off)
        return here.index(fixed)

    def direct_fold(s, p):
        return p >= 1

    def merged(s, p, off):
        index = fold(s, p, off)
        if p == 0:
            mine = held[s][(here.core,) + index + (slice(None), pl.ds(0, WIDTHS[s]))]
            return mine + inner[s][index]
        return inner[s][index]

    def core_copy(s):
        return remote(
            held[s].at[1 - here.core, :, :, :, :, pl.ds(0, WIDTHS[s])],
            inner[s],
            rcore.at[s, 0],
            rcore.at[s, 1],
            here.at(flip=True),
        )

    def produce(s):
        def step(core):
            def one(h, carry):
                i = 2 * core + h
                value = jnp.dot(
                    act[rows_at(i), :], down[:, span(s)], preferred_element_type=jnp.float32
                )
                held[s][core, pl.ds(2 * h, 2), :, :, :, : WIDTHS[s]] = value.astype(jnp.bfloat16).reshape(
                    2, 4, 4, rows, WIDTHS[s]
                )
                return carry

            lax.fori_loop(0, 2, one, 0)

        step(1 - here.core)
        go(core_copy(s))
        step(here.core)

    def half_of(s, ref, index, d):
        return ref.at[index + halves(WIDTHS[s], d)]

    def lead(p):
        return (slice(None),) * (2 - p)

    def far_copy(s, p, d, sending):
        axis = ORDERS[s][2 - p]
        index = fold(s, p, 2)
        if direct_fold(s, p):
            return remote(
                inner[s].at[index], fars[s][p], rfar.at[s, p, 0, 0], rfar.at[s, p, 0, 1], here.at(axis, 2)
            )
        return remote(
            half_of(s, inner[s], index, d),
            half_of(s, fars[s][p], lead(p), d),
            rfar.at[s, p, d, 0],
            rfar.at[s, p, d, 1],
            here.at(axis, (1, 3)[d]),
        )

    def near_copy(s, p, d, h):
        axis = ORDERS[s][2 - p]
        off = (1, 3)[d]
        return remote(
            half_of(s, inner[s], fold(s, p, off), h),
            half_of(s, nears[s][p], (d,) + lead(p), h),
            rnear.at[s, p, d, h, 0],
            rnear.at[s, p, d, h, 1],
            here.at(axis, off),
        )

    def fold_far(s, p):
        if p == 0:
            core_copy(s).wait_recv()
            inner[s][fold(s, 0, 2)] = merged(s, 0, 2)
        for d in range(1 if direct_fold(s, p) else 2):
            go(far_copy(s, p, d, True))
        for d, off in enumerate((1, 3)):
            if p == 0:
                inner[s][fold(s, p, off)] = merged(s, p, off)
            go(near_copy(s, p, d, 1 - d))
            if direct_fold(s, p):
                go(near_copy(s, p, d, d))

    def fold_near(s, p):
        for d, off in enumerate((1, 3)):
            far_copy(s, p, d, False).wait_recv()
            part = fold(s, p, off) + halves(WIDTHS[s], d)
            inner[s][part] = inner[s][part] + fars[s][p][lead(p) + halves(WIDTHS[s], d)]
            go(near_copy(s, p, d, d))

    def fold_end(s, p):
        value = merged(s, p, 0).astype(jnp.float32)
        for d in range(2):
            for h in range(2):
                near_copy(s, p, d, h).wait_recv()
            value = value + nears[s][p][d].astype(jnp.float32)
        if direct_fold(s, p):
            far_copy(s, p, 0, False).wait_recv()
            value = value + fars[s][p][...].astype(jnp.float32)
        if p == 2:
            mixed[:, span(s)] = mixed[:, span(s)] + value
        else:
            inner[s][fold(s, p, 0)] = value.astype(jnp.bfloat16)

    def next_fold(s, p):
        fold_end(s, p - 1)
        fold_far(s, p)

    phases = (
        (produce, 0),
        (lambda s: fold_far(s, 0), 1),
        (lambda s: fold_near(s, 0), 3),
        (lambda s: next_fold(s, 1), 5),
        (lambda s: next_fold(s, 2), 7),
        (lambda s: fold_end(s, 2), 9),
    )
    for step in range(n + phases[-1][1]):
        for phase, lag in phases:
            if 0 <= step - lag < n:
                phase(step - lag)
    for copy in sends:
        copy.wait_send()


def run_layer(queries, new_keys, new_values, cache_keys, cache_values, cache_len, out_proj, resid, gain, router, ids,
              gate_slab, up_slab, down_slab):
    rows, width = resid.shape
    hidden = gate_slab.shape[2]
    n = len(ORDERS)
    dma, bf = pltpu.SemaphoreType.DMA, jnp.bfloat16
    vmem, anywhere = pl.BlockSpec(memory_space=pltpu.VMEM), pl.BlockSpec(memory_space=pl.ANY)
    extra = 128
    shapes = [
        pltpu.VMEM((rows, width + 2 * extra), bf),
        pltpu.VMEM((32, H // 32, rows, HD), bf),
        pltpu.VMEM(cache_keys.shape, bf),
        pltpu.VMEM(cache_values.shape, bf),
        pltpu.VMEM((H * rows, HD), jnp.float32),
        pltpu.VMEM((H * rows, HD), jnp.float32),
        pltpu.VMEM(new_keys.shape, jnp.float32),
        pltpu.VMEM(new_values.shape, jnp.float32),
        pltpu.VMEM(out_proj.shape, bf),
        pltpu.VMEM((32, H // 32, rows, HD), bf),
        pltpu.VMEM((3, 4, rows, width), bf),
        pltpu.VMEM((4, rows, width), bf),
        pltpu.VMEM((3, rows, width), bf),
        dma((3,)),
        dma((32, 2)),
        dma((n, 2)),
        dma((n, 4, 4, 2)),
        dma((n, 4, 2)),
        pltpu.VMEM((gate_slab.shape[1], 2 * hidden), bf),
        pltpu.VMEM(down_slab.shape[1:], bf),
        pltpu.VMEM((128 * rows, hidden), bf),
        pltpu.VMEM((128 * CAP, 2 * hidden), jnp.float32),
        pltpu.VMEM((128 * CAP, max(WIDTHS)), bf),
        pltpu.VMEM((8, 16 * CAP, 16 * rows), bf),
        pltpu.VMEM((8, 16 * rows, 16 * CAP), bf),
        dma((3,)),
        dma((n, 3, 2, 2, 2)),
        dma((n, 3, 2, 2)),
        dma((n, 4, 2)),
        dma((n, 3, 2, 2, 2)),
        dma((n, 3, 2, 2)),
        dma((n, 2)),
    ]
    shapes += [pltpu.VMEM((2, 4, 4, 4, rows, w + extra * (s in (0, n - 1))), bf) for s, w in enumerate(WIDTHS)]
    shapes += [pltpu.VMEM((4, 4, 4, rows, w), bf) for w in WIDTHS]
    shapes += [pltpu.VMEM((2,) + (4,) * (2 - p) + (rows, w), bf) for w in WIDTHS for p in range(3)]
    shapes += [pltpu.VMEM((4,) * (2 - p) + (rows, w), bf) for w in WIDTHS for p in range(3)]
    return pl.pallas_call(
        layer_kernel,
        out_shape=jax.ShapeDtypeStruct((rows, width), jnp.float32),
        in_specs=[vmem, vmem, vmem, anywhere, anywhere, pl.BlockSpec(memory_space=pltpu.SMEM), anywhere]
        + [vmem] * 4
        + [anywhere] * 3,
        out_specs=vmem,
        scratch_shapes=shapes,
        compiler_params=pltpu.CompilerParams(
            collective_id=0, has_side_effects=True, vmem_limit_bytes=VMEM_LIMIT
        ),
    )(
        queries, new_keys, new_values, cache_keys, cache_values, cache_len, out_proj, resid, gain, router, ids,
        gate_slab, up_slab, down_slab,
    )


def local(
    resid,
    queries,
    new_keys,
    new_values,
    cache_keys,
    cache_values,
    cache_len,
    out_proj,
    norm_gain,
    router,
    expert_ids,
    gate_slab,
    up_slab,
    down_slab,
):
    return run_layer(
        queries, new_keys, new_values, cache_keys, cache_values, cache_len, out_proj, resid,
        norm_gain.reshape(1, -1), router.T, expert_ids.T, gate_slab, up_slab, down_slab,
    )


def solution(mesh):
    in_specs = (
        P(("ep", "dp"), None),
        P(("ep", "dp"), None),
        P(("ep", "dp"), None),
        P(("ep", "dp"), None),
        P(("ep", "dp"), None, None),
        P(("ep", "dp"), None, None),
        P(("ep", "dp")),
        P("ep", None),
        P(),
        P(),
        P(("ep", "dp"), None),
        P(("ep", "dp"), None, None),
        P(("ep", "dp"), None, None),
        P(("ep", "dp"), None, None),
    )
    out_specs = P(("ep", "dp"), None)
    return jax.shard_map(local, mesh=mesh, in_specs=in_specs, out_specs=out_specs, check_vma=False)
```

```python
import math

import jax
import jax.numpy as jnp
from jax import lax
from jax.experimental import pallas as pl
from jax.experimental.pallas import tpu as pltpu
from jax.sharding import PartitionSpec as P

D = 4096
H = 64
KVH = 4
HD = 128
TOP = 8
CAP = 4


MESH = pl.DeviceIdType.MESH
VMEM_LIMIT = 66_000_000


def remote(src, dst, send, recv, device):
    return pltpu.make_async_remote_copy(
        src_ref=src, dst_ref=dst, send_sem=send, recv_sem=recv, device_id=device, device_id_type=MESH
    )


def attend(queries, new_keys, new_values, keys, values, lengths, attended, qs, os, nk, nv):
    tokens = queries.shape[0]
    share = H // KVH
    scale = 1.0 / math.sqrt(HD)
    for h in range(H):
        qs[tokens * h : tokens * h + tokens, :] = queries[:, HD * h : HD * h + HD].astype(jnp.float32)
    nk[...] = new_keys[...].astype(jnp.float32)
    nv[...] = new_values[...].astype(jnp.float32)

    def spread(row):
        return jnp.concatenate(
            [jnp.broadcast_to(row[:, HD * g : HD * g + HD], (share, HD)) for g in range(KVH)], axis=0
        )

    def one(t):
        rows = pl.ds(t, H, stride=tokens)
        query = qs[rows, :]
        narrow = query.astype(jnp.bfloat16)
        scores = jnp.concatenate(
            [
                lax.dot_general(
                    narrow[share * g : share * g + share],
                    keys[t, :, HD * g : HD * g + HD],
                    (((1,), (1,)), ((), ())),
                    preferred_element_type=jnp.float32,
                )
                for g in range(KVH)
            ],
            axis=0,
        )
        own = jnp.sum(query * spread(nk[pl.ds(t, 1), :]), axis=1, keepdims=True) * scale
        valid = lax.broadcasted_iota(jnp.int32, scores.shape, 1) < lengths[t]
        scores = jnp.where(valid, scores * scale, -1e30)
        peak = jnp.maximum(jnp.max(scores, axis=1, keepdims=True), own)
        grown = jnp.exp(scores - peak)
        own_grown = jnp.exp(own - peak)
        denom = jnp.sum(grown, axis=1, keepdims=True) + own_grown
        weights = (grown / denom).astype(jnp.bfloat16)
        own_weight = (own_grown / denom).astype(jnp.bfloat16).astype(jnp.float32)
        blended = jnp.concatenate(
            [
                jnp.dot(
                    weights[share * g : share * g + share],
                    values[t, :, HD * g : HD * g + HD],
                    preferred_element_type=jnp.float32,
                )
                for g in range(KVH)
            ],
            axis=0,
        )
        os[rows, :] = blended + own_weight * spread(nv[pl.ds(t, 1), :])

    def several(i, carry):
        for k in range(8):
            one(8 * i + k)
        return carry

    lax.fori_loop(0, tokens // 8, several, 0)
    attended[...] = os[...].astype(jnp.bfloat16).reshape(attended.shape)


AXES = ("y", "x", "z")
TURNS = (("x", "y", "z"), ("y", "z", "x"), ("z", "x", "y"))
ORDERS = TURNS * 3
WIDTHS = (512,) * 6 + (384, 384, 256)
STARTS = tuple(sum(WIDTHS[:s]) for s in range(len(WIDTHS)))


class Spot:
    def __init__(self):
        ep = lax.axis_index("ep")
        self.core = lax.rem(ep, 2)
        self.pos = {"x": lax.rem(ep // 2, 4), "y": ep // 8, "z": lax.axis_index("dp")}

    def coord(self, axis, off):
        return lax.rem(self.pos[axis] + off, 4) if off else self.pos[axis]

    def at(self, axis=None, off=0, flip=False):
        place = dict(self.pos)
        if axis:
            place[axis] = self.coord(axis, off)
        core = 1 - self.core if flip else self.core
        return ((place["y"] * 4 + place["x"]) * 2 + core, place["z"])

    def plane(self, dy, dx):
        return ((self.coord("y", dy) * 4 + self.coord("x", dx)) * 2 + self.core, self.pos["z"])

    def index(self, fixed):
        return tuple(fixed.get(axis, slice(None)) for axis in AXES)


LAGS = (0, 2, 5, 8)


def layer_kernel(
    queries, new_keys, new_values, keys_hbm, values_hbm, lengths, weight_hbm, resid, gain, router, ids,
    gate_hbm, up_hbm, down_hbm, mixed,
    own, attended, keys, values, qs, os, nk, nv, weight, regrouped, in2, sum2, in3, asem, osem, psem, qsem, tsem,
    gu, down, act, total, picked, sel, back, wsem, nsem, fsem, csem, rnear, rfar, rcore, *scratch
):
    n = len(ORDERS)
    held, inner = scratch[:n], scratch[n : 2 * n]
    nears = [scratch[2 * n + 3 * s : 2 * n + 3 * s + 3] for s in range(n)]
    fars = [scratch[5 * n + 3 * s : 5 * n + 3 * s + 3] for s in range(n)]
    here = Spot()
    rows = own.shape[0]
    hidden = act.shape[1]
    experts = router.shape[0]
    count = 32
    ep, z = lax.axis_index("ep"), lax.axis_index("dp")
    caches = [
        pltpu.make_async_copy(keys_hbm, keys, asem.at[0]),
        pltpu.make_async_copy(values_hbm, values, asem.at[1]),
        pltpu.make_async_copy(weight_hbm, weight, asem.at[2]),
    ]
    loads = [
        pltpu.make_async_copy(gate_hbm.at[0], gu.at[:, pl.ds(0, hidden)], wsem.at[0]),
        pltpu.make_async_copy(up_hbm.at[0], gu.at[:, pl.ds(hidden, hidden)], wsem.at[1]),
        pltpu.make_async_copy(down_hbm.at[0], down, wsem.at[2]),
    ]
    for load in caches + loads:
        load.start()

    def peer(j):
        return lax.rem(ep + j, count)

    barrier = pltpu.get_barrier_semaphore()
    everyone = [(peer(j), z) for j in range(1, count)] + [here.at("z", off) for off in (1, 2, 3)]
    for device in everyone:
        pl.semaphore_signal(barrier, inc=1, device_id=device, device_id_type=MESH)
    caches[0].wait()
    caches[1].wait()
    attend(queries, new_keys, new_values, keys, values, lengths, attended, qs, os, nk, nv)
    pl.semaphore_wait(barrier, len(everyone))
    sends, early = [], []

    def go(copy, kept=sends):
        copy.start()
        kept.append(copy)

    for j in range(1, count):
        go(remote(attended.at[peer(j)], regrouped.at[ep], osem.at[j, 0], osem.at[count - j, 1], (peer(j), z)), early)
    regrouped[ep] = attended[ep]
    caches[2].wait()
    for j in range(1, count):
        remote(attended.at[peer(j)], regrouped.at[peer(j)], osem.at[j, 0], osem.at[j, 1], (peer(j), z)).wait_recv()

    def pair_copy(s):
        return remote(
            inner[s].at[:, :, 1 - here.core], inner[s].at[:, :, 2], psem.at[s, 0], psem.at[s, 1], here.at(flip=True)
        )

    def turn(s, a, b):
        return (a, b) if s % 2 == 0 else (b, a)

    def line(s, a, b):
        dy, dx = turn(s, a, b)
        return here.coord("y", dy), here.coord("x", dx)

    def columns(s):
        return pl.ds(STARTS[s], WIDTHS[s])

    def first_copy(s, ja, kb, sending):
        y, x = line(s, ja, kb)
        return remote(
            inner[s].at[y, x, 2],
            in2.at[3 - ja, kb, :, columns(s)],
            qsem.at[s, ja, kb, 0],
            qsem.at[s, 4 - ja if sending else ja, kb, 1],
            here.plane(*turn(s, ja, 0)),
        )

    def second_copy(s, kb, sending):
        return remote(
            sum2.at[kb, :, columns(s)],
            in3.at[3 - kb, :, columns(s)],
            tsem.at[s, kb, 0],
            tsem.at[s, 4 - kb if sending else kb, 1],
            here.plane(*turn(s, 0, kb)),
        )

    def wide(value):
        return value.astype(jnp.float32)

    def phase0(s):
        left = jnp.concatenate([regrouped[:, k].reshape(count * rows, HD) for k in range(2)], axis=1)
        value = jnp.dot(left, weight[:, columns(s)], preferred_element_type=jnp.float32)
        inner[s][:, :, 0:2] = value.astype(jnp.bfloat16).reshape(4, 4, 2, rows, WIDTHS[s])
        go(pair_copy(s), early)

    def phase1(s):
        pair_copy(s).wait_recv()
        for a in (1, 2, 3, 0):
            for b in (1, 2, 3, 0):
                y, x = line(s, a, b)
                inner[s][y, x, 2] = (wide(inner[s][y, x, here.core]) + wide(inner[s][y, x, 2])).astype(jnp.bfloat16)
                if a:
                    go(first_copy(s, a, b, True), early)

    def phase2(s):
        for b in (1, 2, 3, 0):
            y, x = line(s, 0, b)
            value = wide(inner[s][y, x, 2])
            for a in range(1, 4):
                first_copy(s, a, b, False).wait_recv()
                value = value + wide(in2[a - 1, b, :, columns(s)])
            sum2[b, :, columns(s)] = value.astype(jnp.bfloat16)
            if b:
                go(second_copy(s, b, True), early)

    def phase3(s):
        value = wide(sum2[0, :, columns(s)])
        for b in range(1, 4):
            second_copy(s, b, False).wait_recv()
            value = value + wide(in3[b - 1, :, columns(s)])
        value = wide(resid[:, columns(s)]) + value
        mixed[:, columns(s)] = value
        squares.append(jnp.sum(value * value, axis=1, keepdims=True))
        scaled = (value * gain[:, columns(s)]).astype(jnp.bfloat16)
        own[:, columns(s)] = scaled
        logits.append(
            lax.dot_general(scaled, router[:, columns(s)], (((1,), (1,)), ((), ())), preferred_element_type=jnp.float32)
        )
        if s < n - 1:
            start(s)
        if s >= 3:
            second(s - 3)
        if s >= 6:
            second_far(s - 6)
            third(s - 6)

    def find():
        label = lax.broadcasted_iota(jnp.int32, (experts, rows), 0)
        marks = sum((ids[k : k + 1, :] == label).astype(jnp.float32) for k in range(TOP))
        eye = (
            lax.broadcasted_iota(jnp.int32, (rows, rows), 0) == lax.broadcasted_iota(jnp.int32, (rows, rows), 1)
        ).astype(jnp.float32)
        return lax.dot_general(eye, marks, (((1,), (1,)), ((), ())), preferred_element_type=jnp.float32) > 0.5

    def route(named, logit):
        peak = jnp.max(jnp.where(named, logit, -jnp.inf), axis=1, keepdims=True)
        grown = jnp.where(named, jnp.exp(jnp.where(named, logit - peak, 0.0)), 0.0)
        return grown / jnp.sum(grown, axis=1, keepdims=True)

    def halves(width, d):
        cut = 256 if width > 256 else 128
        return (slice(None), pl.ds(0, cut) if d == 0 else pl.ds(cut, width - cut))

    def spread_index(s, p, off, core=None):
        order = ORDERS[s]
        fixed = {axis: here.pos[axis] for axis in order[p + 1 :]}
        fixed[order[p]] = here.coord(order[p], off)
        return (here.core if core is None else core,) + here.index(fixed)

    def spread(s, p, off, core=None):
        return held[s].at[spread_index(s, p, off, core)]

    def spread_half(s, p, off, d):
        width = held[s].shape[-1]
        return held[s].at[spread_index(s, p, off) + halves(width, d)]

    def direct_gather(s, p):
        return p == 0 or (p == 1 and s < 3) or (p == 2 and s >= 6)

    def near_gather(s, p, d, h, sending):
        axis = ORDERS[s][p]
        off = (1, 3)[d]
        ref = spread_half(s, p, 0 if sending else 4 - off, h)
        return remote(
            ref, ref, nsem.at[s, p, d, h, 0], nsem.at[s, p, d, h, 1], here.at(axis, off if sending else 4 - off)
        )

    def gather_near(s, p):
        axis = ORDERS[s][p]
        for h in range(2):
            for d in range(2):
                go(near_gather(s, p, d, (d + h) % 2, True))
        if direct_gather(s, p):
            ref = spread(s, p, 0)
            go(remote(ref, ref, fsem.at[s, p, 0, 0], fsem.at[s, p, 0, 1], here.at(axis, 2)))
        if p == 2:
            give(s, 0, 0)

    def gather_far(s, p):
        axis = ORDERS[s][p]
        for d, (off, back) in enumerate(((1, 3), (3, 1))):
            near_gather(s, p, d, d, False).wait_recv()
            if not direct_gather(s, p):
                ref = spread_half(s, p, back, d)
                go(remote(ref, ref, fsem.at[s, p, d, 0], fsem.at[s, p, d, 1], here.at(axis, off)))

    def gather_end(s, p):
        axis = ORDERS[s][p]
        for d, back in enumerate((3, 1)):
            near_gather(s, p, d, 1 - d, False).wait_recv()
            if p == 2:
                give(s, 1 + d, back)
        if direct_gather(s, p):
            ref = spread(s, p, 2)
            remote(ref, ref, fsem.at[s, p, 0, 0], fsem.at[s, p, 0, 1], here.at(axis, 2)).wait_recv()
        else:
            for d, back in enumerate((3, 1)):
                ref = spread_half(s, p, 2, d)
                remote(ref, ref, fsem.at[s, p, d, 0], fsem.at[s, p, d, 1], here.at(axis, back)).wait_recv()
        if p == 2:
            give(s, 3, 2)

    def give(s, k, off):
        ref = spread(s, 2, off)
        go(remote(ref, ref, csem.at[s, k, 0], csem.at[s, k, 1], here.at(flip=True)))

    def take(s):
        for k, off in enumerate((0, 3, 1, 2)):
            ref = spread(s, 2, off, 1 - here.core)
            remote(ref, ref, csem.at[s, k, 0], csem.at[s, k, 1], here.at(flip=True)).wait_recv()

    group = 32 * rows
    block = 16 * rows
    slots = 16 * CAP
    mine = (ep * 4 + z) // 2

    def rows_at(i):
        return pl.ds(pl.multiple_of(i * group, group), group)

    def span(s):
        return slice(STARTS[s], STARTS[s] + WIDTHS[s])

    def lane_of(value, wanted):
        lane = lax.broadcasted_iota(jnp.int32, value.shape, 1)
        return jnp.sum(jnp.where(wanted(lane), value, 0.0), axis=1, keepdims=True)

    def select():
        row = lax.broadcasted_iota(jnp.int32, (block, block), 0)
        col = lax.broadcasted_iota(jnp.int32, (block, block), 1)
        earlier = ((row // rows == col // rows) & (col < row)).astype(jnp.bfloat16)
        token = lax.broadcasted_iota(jnp.int32, (block, slots), 0)
        slot = lax.broadcasted_iota(jnp.int32, (block, slots), 1)
        near = token // rows == slot // CAP
        turn_of = lax.rem(slot, CAP).astype(jnp.float32)
        eye = (
            lax.broadcasted_iota(jnp.int32, (slots, slots), 0) == lax.broadcasted_iota(jnp.int32, (slots, slots), 1)
        ).astype(jnp.bfloat16)

        def one(i, carry):
            marks = held[0][i // 4, lax.rem(i, 4), :, :, :, WIDTHS[0] :].reshape(block, 128)
            rank = lane_of(
                jnp.dot(earlier, marks, preferred_element_type=jnp.float32), lambda lane: lane == mine
            )
            chosen = lane_of(marks.astype(jnp.float32), lambda lane: lane == mine)
            hit = jnp.where(near & (rank == turn_of), chosen, 0.0).astype(jnp.bfloat16)
            back[i] = hit
            sel[i] = lax.dot_general(
                eye, hit, (((1,), (1,)), ((), ())), preferred_element_type=jnp.float32
            ).astype(jnp.bfloat16)
            return carry

        lax.fori_loop(0, 8, one, 0)

    def tokens_of(s, i, cols):
        return held[s][i // 4, i % 4, :, :, :, cols].reshape(block, cols.stop - cols.start)

    def consume(s):
        if s == 0:
            select()
            loads[0].wait()
            loads[1].wait()
        width = WIDTHS[s]
        for i in range(8):
            chosen = jnp.dot(sel[i], tokens_of(s, i, slice(0, width)), preferred_element_type=jnp.float32)
            picked[slots * i : slots * i + slots, :width] = chosen.astype(jnp.bfloat16)
        for i in range(2):
            part = slice(4 * slots * i, 4 * slots * (i + 1))
            value = jnp.dot(picked[part, :width], gu[span(s), :], preferred_element_type=jnp.float32)
            total[part, :] = value if s == 0 else total[part, :] + value

    def start(s):
        place = (here.core, here.pos["y"], here.pos["x"], here.pos["z"], slice(None))
        held[s][place + (pl.ds(0, WIDTHS[s]),)] = own[:, columns(s)]
        if s == 0:
            held[s][place + (pl.ds(WIDTHS[s], 128),)] = own[:, pl.ds(D, 128)]
        if s == n - 1:
            held[s][place + (pl.ds(WIDTHS[s], 128),)] = own[:, pl.ds(D + 128, 128)]
        gather_near(s, 0)

    def second(s):
        gather_far(s, 0)
        gather_end(s, 0)
        gather_near(s, 1)

    def second_far(s):
        gather_far(s, 1)

    def third(s):
        gather_end(s, 1)
        gather_near(s, 2)

    def third_far(s):
        gather_far(s, 2)

    def last(s):
        gather_end(s, 2)

    def use(s):
        take(s)
        consume(s)

    def run(*steps):
        for phase, group_of in steps:
            for s in group_of:
                phase(s)

    squares, logits = [], []
    named = find()
    own[:, D : D + 128] = jnp.concatenate(
        [named.astype(jnp.float32), jnp.zeros((rows, 128 - experts), jnp.float32)], axis=1
    ).astype(jnp.bfloat16)
    for step in range(n + LAGS[-1]):
        for phase, lag in zip((phase0, phase1, phase2, phase3), LAGS):
            if 0 <= step - lag < n:
                phase(step - lag)
    for copy in early:
        copy.wait_send()
    scale = lax.rsqrt(jnp.maximum(sum(squares) / D, 0.25))
    probs = route(named, sum(logits) * scale)
    high = scale.astype(jnp.bfloat16)
    low = scale - high.astype(jnp.float32)
    lane = lax.broadcasted_iota(jnp.int32, (rows, 128 - experts), 1)
    tail = jnp.where(lane == 0, high.astype(jnp.float32), jnp.where(lane == 1, low, 0.0))
    own[:, D + 128 :] = jnp.concatenate([probs, tail], axis=1).astype(jnp.bfloat16)
    run(
        (start, (8,)), (second_far, (3, 4, 5)), (second, (6, 7, 8)), (third_far, (0, 1, 2)), (third, (3, 4, 5)),
        (second_far, (6, 7, 8)), (last, (0, 1, 2)),
    )
    for s in range(3):
        run((use, (s,)), (third_far, (3 + s,)), (third, (6 + s,)))
    run((last, (3, 4, 5)))
    for s in range(3, 6):
        run((use, (s,)), (third_far, (3 + s,)))
    run((last, (6, 7, 8)), (use, (6, 7, 8)))
    for copy in sends:
        copy.wait_send()
    sends.clear()
    loads[2].wait()
    for i in range(8):
        tail = tokens_of(n - 1, i, slice(WIDTHS[n - 1], WIDTHS[n - 1] + 128))
        tail = jnp.dot(sel[i], tail, preferred_element_type=jnp.float32)
        prob = lane_of(tail, lambda lane: lane == mine)
        factor = lane_of(tail, lambda lane: lane // 2 == experts // 2)
        part = slice(slots * i, slots * i + slots)
        gate_val = total[part, :hidden] * factor
        value = gate_val / (1.0 + jnp.exp(-gate_val)) * (total[part, hidden:] * factor) * prob
        act[block * i : block * i + block, :] = jnp.dot(
            back[i], value.astype(jnp.bfloat16), preferred_element_type=jnp.float32
        ).astype(jnp.bfloat16)

    def fold(s, p, off):
        order = ORDERS[s][::-1]
        fixed = {axis: here.pos[axis] for axis in order[:p]}
        fixed[order[p]] = here.coord(order[p], off)
        return here.index(fixed)

    def direct_fold(s, p):
        return p >= 1

    def merged(s, p, off):
        index = fold(s, p, off)
        if p == 0:
            mine = held[s][(here.core,) + index + (slice(None), pl.ds(0, WIDTHS[s]))]
            return mine + inner[s][index]
        return inner[s][index]

    def core_copy(s):
        return remote(
            held[s].at[1 - here.core, :, :, :, :, pl.ds(0, WIDTHS[s])],
            inner[s],
            rcore.at[s, 0],
            rcore.at[s, 1],
            here.at(flip=True),
        )

    def produce(s):
        def step(core):
            def one(h, carry):
                i = 2 * core + h
                value = jnp.dot(
                    act[rows_at(i), :], down[:, span(s)], preferred_element_type=jnp.float32
                )
                held[s][core, pl.ds(2 * h, 2), :, :, :, : WIDTHS[s]] = value.astype(jnp.bfloat16).reshape(
                    2, 4, 4, rows, WIDTHS[s]
                )
                return carry

            lax.fori_loop(0, 2, one, 0)

        step(1 - here.core)
        go(core_copy(s))
        step(here.core)

    def half_of(s, ref, index, d):
        return ref.at[index + halves(WIDTHS[s], d)]

    def lead(p):
        return (slice(None),) * (2 - p)

    def far_copy(s, p, d, sending):
        axis = ORDERS[s][2 - p]
        index = fold(s, p, 2)
        if direct_fold(s, p):
            return remote(
                inner[s].at[index], fars[s][p], rfar.at[s, p, 0, 0], rfar.at[s, p, 0, 1], here.at(axis, 2)
            )
        return remote(
            half_of(s, inner[s], index, d),
            half_of(s, fars[s][p], lead(p), d),
            rfar.at[s, p, d, 0],
            rfar.at[s, p, d, 1],
            here.at(axis, (1, 3)[d]),
        )

    def near_copy(s, p, d, h):
        axis = ORDERS[s][2 - p]
        off = (1, 3)[d]
        return remote(
            half_of(s, inner[s], fold(s, p, off), h),
            half_of(s, nears[s][p], (d,) + lead(p), h),
            rnear.at[s, p, d, h, 0],
            rnear.at[s, p, d, h, 1],
            here.at(axis, off),
        )

    def fold_far(s, p):
        if p == 0:
            core_copy(s).wait_recv()
            inner[s][fold(s, 0, 2)] = merged(s, 0, 2)
        for d in range(1 if direct_fold(s, p) else 2):
            go(far_copy(s, p, d, True))
        for d, off in enumerate((1, 3)):
            if p == 0:
                inner[s][fold(s, p, off)] = merged(s, p, off)
            go(near_copy(s, p, d, 1 - d))
            if direct_fold(s, p):
                go(near_copy(s, p, d, d))

    def fold_near(s, p):
        for d, off in enumerate((1, 3)):
            far_copy(s, p, d, False).wait_recv()
            part = fold(s, p, off) + halves(WIDTHS[s], d)
            inner[s][part] = inner[s][part] + fars[s][p][lead(p) + halves(WIDTHS[s], d)]
            go(near_copy(s, p, d, d))

    def fold_end(s, p):
        value = merged(s, p, 0).astype(jnp.float32)
        for d in range(2):
            for h in range(2):
                near_copy(s, p, d, h).wait_recv()
            value = value + nears[s][p][d].astype(jnp.float32)
        if direct_fold(s, p):
            far_copy(s, p, 0, False).wait_recv()
            value = value + fars[s][p][...].astype(jnp.float32)
        if p == 2:
            mixed[:, span(s)] = mixed[:, span(s)] + value
        else:
            inner[s][fold(s, p, 0)] = value.astype(jnp.bfloat16)

    def next_fold(s, p):
        fold_end(s, p - 1)
        fold_far(s, p)

    phases = (
        (produce, 0),
        (lambda s: fold_far(s, 0), 1),
        (lambda s: fold_near(s, 0), 3),
        (lambda s: next_fold(s, 1), 5),
        (lambda s: next_fold(s, 2), 7),
        (lambda s: fold_end(s, 2), 9),
    )
    for step in range(n + phases[-1][1]):
        for phase, lag in phases:
            if 0 <= step - lag < n:
                phase(step - lag)
    for copy in sends:
        copy.wait_send()


def run_layer(queries, new_keys, new_values, cache_keys, cache_values, cache_len, out_proj, resid, gain, router, ids,
              gate_slab, up_slab, down_slab):
    rows, width = resid.shape
    hidden = gate_slab.shape[2]
    n = len(ORDERS)
    dma, bf = pltpu.SemaphoreType.DMA, jnp.bfloat16
    vmem, anywhere = pl.BlockSpec(memory_space=pltpu.VMEM), pl.BlockSpec(memory_space=pl.ANY)
    extra = 128
    shapes = [
        pltpu.VMEM((rows, width + 2 * extra), bf),
        pltpu.VMEM((32, H // 32, rows, HD), bf),
        pltpu.VMEM(cache_keys.shape, bf),
        pltpu.VMEM(cache_values.shape, bf),
        pltpu.VMEM((H * rows, HD), jnp.float32),
        pltpu.VMEM((H * rows, HD), jnp.float32),
        pltpu.VMEM(new_keys.shape, jnp.float32),
        pltpu.VMEM(new_values.shape, jnp.float32),
        pltpu.VMEM(out_proj.shape, bf),
        pltpu.VMEM((32, H // 32, rows, HD), bf),
        pltpu.VMEM((3, 4, rows, width), bf),
        pltpu.VMEM((4, rows, width), bf),
        pltpu.VMEM((3, rows, width), bf),
        dma((3,)),
        dma((32, 2)),
        dma((n, 2)),
        dma((n, 4, 4, 2)),
        dma((n, 4, 2)),
        pltpu.VMEM((gate_slab.shape[1], 2 * hidden), bf),
        pltpu.VMEM(down_slab.shape[1:], bf),
        pltpu.VMEM((128 * rows, hidden), bf),
        pltpu.VMEM((128 * CAP, 2 * hidden), jnp.float32),
        pltpu.VMEM((128 * CAP, max(WIDTHS)), bf),
        pltpu.VMEM((8, 16 * CAP, 16 * rows), bf),
        pltpu.VMEM((8, 16 * rows, 16 * CAP), bf),
        dma((3,)),
        dma((n, 3, 2, 2, 2)),
        dma((n, 3, 2, 2)),
        dma((n, 4, 2)),
        dma((n, 3, 2, 2, 2)),
        dma((n, 3, 2, 2)),
        dma((n, 2)),
    ]
    shapes += [pltpu.VMEM((2, 4, 4, 4, rows, w + extra * (s in (0, n - 1))), bf) for s, w in enumerate(WIDTHS)]
    shapes += [pltpu.VMEM((4, 4, 4, rows, w), bf) for w in WIDTHS]
    shapes += [pltpu.VMEM((2,) + (4,) * (2 - p) + (rows, w), bf) for w in WIDTHS for p in range(3)]
    shapes += [pltpu.VMEM((4,) * (2 - p) + (rows, w), bf) for w in WIDTHS for p in range(3)]
    return pl.pallas_call(
        layer_kernel,
        out_shape=jax.ShapeDtypeStruct((rows, width), jnp.float32),
        in_specs=[vmem, vmem, vmem, anywhere, anywhere, pl.BlockSpec(memory_space=pltpu.SMEM), anywhere]
        + [vmem] * 4
        + [anywhere] * 3,
        out_specs=vmem,
        scratch_shapes=shapes,
        compiler_params=pltpu.CompilerParams(
            collective_id=0, has_side_effects=True, vmem_limit_bytes=VMEM_LIMIT
        ),
    )(
        queries, new_keys, new_values, cache_keys, cache_values, cache_len, out_proj, resid, gain, router, ids,
        gate_slab, up_slab, down_slab,
    )


def local(
    resid,
    queries,
    new_keys,
    new_values,
    cache_keys,
    cache_values,
    cache_len,
    out_proj,
    norm_gain,
    router,
    expert_ids,
    gate_slab,
    up_slab,
    down_slab,
):
    return run_layer(
        queries, new_keys, new_values, cache_keys, cache_values, cache_len, out_proj, resid,
        norm_gain.reshape(1, -1), router.T, expert_ids.T, gate_slab, up_slab, down_slab,
    )


def solution(mesh):
    in_specs = (
        P(("ep", "dp"), None),
        P(("ep", "dp"), None),
        P(("ep", "dp"), None),
        P(("ep", "dp"), None),
        P(("ep", "dp"), None, None),
        P(("ep", "dp"), None, None),
        P(("ep", "dp")),
        P("ep", None),
        P(),
        P(),
        P(("ep", "dp"), None),
        P(("ep", "dp"), None, None),
        P(("ep", "dp"), None, None),
        P(("ep", "dp"), None, None),
    )
    out_specs = P(("ep", "dp"), None)
    return jax.shard_map(local, mesh=mesh, in_specs=in_specs, out_specs=out_specs, check_vma=False)
```
